32 devices in a mesh: replica: 4 (over y, x), fsdp: 8 (over z, core).
Axes of the slice: x: 2, y: 2, z: 4, core: 2. Of those that a mesh axis runs over, the one named last changes fastest.
Arguments:
- codes: int32 [4, 8192, 4096], P('replica', None, 'fsdp'), may hold values from -127 to 127
- scales: float32 [4, 32, 8192], P('replica', 'fsdp'), may hold values from 0.002 to 0.03
- master: float32 [8192, 4096], P(('replica', 'fsdp')), may hold values from -6 to 6
- momentum: float32 [8192, 4096], P(('replica', 'fsdp')), may hold values from -6 to 6
Outputs:
- new_master: float32 [8192, 4096], P(('replica', 'fsdp'))
- new_momentum: float32 [8192, 4096], P(('replica', 'fsdp'))
- weights: bfloat16 [8192, 4096], P(None, 'fsdp')
The draws below stay inside these ranges and needn't reach their ends.
All inputs are finite; a program needn't handle non-finite values.
Results may differ from the reference program's by a relative error of at most 0.0075.
Values may be sent and summed in bfloat16 or wider, within the bound.
A program may use at most 128 MiB of HBM per device.

```python
import math
import jax
import jax.numpy as jnp
from jax import lax

D = 4096
FF = 8192
BLOCK = 128
REPLICAS = 4
N_REPLICA = 4


def place_ends(entries, key, least, high):
    shape = entries.shape
    spot = [jax.random.randint(jax.random.fold_in(key, axis), (), 0, shape[axis]) for axis in range(len(shape))]
    entries = entries.at[tuple(spot)].set(least)
    longest = shape.index(max(shape))
    spot[longest] = (spot[longest] + 1) % shape[longest]
    return entries.at[tuple(spot)].set(high)


def block_scale(stream_key, extent, cuts, low, top_value):
    def one(dim, blocks):
        steps = jax.random.uniform(jax.random.fold_in(jax.random.fold_in(stream_key, 6), dim), (blocks,), jnp.float32, low / len(cuts), top_value / len(cuts))
        return jnp.repeat(jnp.exp(steps), extent[dim] // blocks).reshape((-1,) + (1,) * (len(extent) - dim - 1))

    loudness = one(*cuts[0])
    for cut in cuts[1:]:
        loudness = loudness * one(*cut)
    return loudness


def noise(stream_key, extent, width, limit, split=(), held_as=jnp.bfloat16):
    entries = width * jax.random.normal(stream_key, extent, jnp.float32)
    if split:
        entries = entries * block_scale(stream_key, extent, split, -0.22, 0.18)
    return jnp.clip(entries, -limit, limit).astype(held_as)


def setup_inputs(seed: int = 0) -> dict:
    seeds = jax.random.split(jax.random.key(seed), 5)
    codes = place_ends(jax.random.randint(seeds[0], (REPLICAS, FF, D), -127, 128), jax.random.fold_in(seeds[0], 1), -127, 127).astype(jnp.int32)
    scales = jnp.clip(jnp.exp(math.log(0.03) - 2.70805 * jax.random.uniform(seeds[1], (REPLICAS, D // BLOCK, FF), jnp.float32) ** block_scale(seeds[1], (REPLICAS, D // BLOCK, FF), ((0, 4), (1, 8)), -0.2, 0.2)), 0.002, 0.03)
    master = noise(seeds[2], (FF, D), 1.0, 6.0, ((0, 32),), jnp.float32)
    momentum = noise(seeds[3], (FF, D), 0.5, 6.0, ((0, 32),), jnp.float32)
    return {"codes": codes, "scales": scales, "master": master, "momentum": momentum}


outer_rate = 0.7
momentum_factor = 0.9


def reference(codes, scales, master, momentum):
    def add_worker(replica_index, running):
        quantized = lax.dynamic_index_in_dim(codes, replica_index, 0, keepdims=False).astype(jnp.float32)
        scale_rows = lax.dynamic_index_in_dim(scales, replica_index, 0, keepdims=False)
        block_count = scale_rows.shape[0]
        dequantized = quantized.reshape(FF, block_count, BLOCK) * jnp.transpose(scale_rows)[:, :, None]
        return running + dequantized.reshape(FF, D)

    summed = lax.fori_loop(0, N_REPLICA, add_worker, jnp.zeros((FF, D), jnp.float32))
    mean_delta = summed / N_REPLICA
    new_momentum = momentum_factor * momentum + mean_delta
    new_master = master - outer_rate * (mean_delta + momentum_factor * new_momentum)
    weights = new_master.astype(jnp.bfloat16)
    return (new_master, new_momentum, weights)
```

```python
import functools

import jax
import jax.numpy as jnp
from jax import lax
from jax.experimental import pallas as pl
from jax.experimental.pallas import tpu as pltpu
from jax.sharding import PartitionSpec as P

MESH = pl.DeviceIdType.MESH

outer_rate = 0.7
momentum_factor = 0.9

LAGS = (0, 3, 6, 8, 10, 13, 16)
RS1, RS2, X1, X2, AG1, AG2 = range(6)


def kernel(cfg, codes, scales, master, momentum, new_master, new_momentum, weights,
           delta, rs1e, rs1o, rs2e, rs2o, part, got, wsend, cbuf, flat, sbuf,
           send_sem, recv_sem, in_sem, state_sem, near_sem, far_sem):
    A, B, F, K, sub, width, blocks = cfg
    R, block = A * B, width // blocks
    r, f = lax.axis_index("replica"), lax.axis_index("fsdp")
    a, b = r // B, lax.rem(r, B)
    odd_core = lax.rem(f, 2)
    partner = (r, f + 1 - 2 * odd_core)

    def a_peer(i):
        return lax.rem(a + 1 + i, A)

    def b_peer(i):
        return lax.rem(b + 1 + i, B)

    def f_peer(i):
        return lax.rem(f + 1 + i, F)

    barrier = pltpu.get_barrier_semaphore()
    near = f - odd_core + 1
    for i in range(A - 1):
        pl.semaphore_signal(barrier, inc=1, device_id=(a_peer(i) * B + b, near), device_id_type=MESH)
    for i in range(B - 1):
        pl.semaphore_signal(barrier, inc=1, device_id=(a * B + b_peer(i), near), device_id_type=MESH)

    @pl.when(odd_core == 0)
    def _():
        pl.semaphore_signal(barrier, inc=1, device_id=partner, device_id_type=MESH)

    def load(k):
        slot = lax.rem(k, 2)
        return tuple(
            pltpu.make_async_copy(codes.at[pl.ds(q * F, F), k], cbuf.at[slot, pl.ds(q * F, F)], in_sem.at[slot, q])
            for q in range(R)
        )

    scales_in = pltpu.make_async_copy(scales.at[0], flat.at[pl.ds(0, blocks)], state_sem.at[2])
    scales_in.start()
    for k in range(min(2, K)):
        for copy in load(k):
            copy.start()

    for i in range(F // 2 - 1):
        pair = lax.rem(f // 2 + 1 + i, F // 2)
        pl.semaphore_signal(barrier, inc=1, device_id=(r, 2 * pair), device_id_type=MESH)

    state_in = (
        pltpu.make_async_copy(master, new_master, state_sem.at[0]),
        pltpu.make_async_copy(momentum, new_momentum, state_sem.at[1]),
    )

    def turn(i, carry):
        tile = flat[:, pl.ds(pl.multiple_of(i * 128, 128), 128)]
        sbuf[pl.ds(pl.multiple_of(i * 128, 128), 128), :] = jnp.transpose(tile)
        return carry

    scales_in.wait()
    lax.fori_loop(0, flat.shape[1] // 128, turn, 0, unroll=8)

    def send(stage, k, src, dst, device):
        pltpu.make_async_remote_copy(
            src_ref=src, dst_ref=dst, send_sem=send_sem.at[stage, k], recv_sem=recv_sem.at[stage, k],
            device_id=device, device_id_type=MESH,
        ).start()

    def wait_bytes(sem, stage, k, ref):
        pltpu.make_async_copy(ref, ref, sem.at[stage, k]).wait()

    def rows(j):
        return pl.ds(pl.multiple_of(j * sub, sub), sub)

    def f32(x):
        return x.astype(jnp.float32)

    def amount(stage, k, even):
        if stage == RS1:
            return rs1e.at[k // 2] if even else rs1o.at[k // 2]
        if stage == RS2:
            return rs2e.at[k // 2] if even else rs2o.at[k // 2]
        if stage in (X1, X2):
            return part.at[k, pl.ds(0, (F - 1) * sub)]
        first, second = (B - 1, B * (A - 1)) if even else (A - 1, A * (B - 1))
        count = first if stage == AG1 else second
        return delta.at[k, pl.ds(0, count)]

    def by_parity(k, fn):
        @pl.when(lax.rem(k, 2) == 0)
        def _():
            fn(True)

        if K > 1:
            @pl.when(lax.rem(k, 2) == 1)
            def _():
                fn(False)

    def scale_codes(k):
        slot = lax.rem(k, 2)
        for copy in load(k):
            copy.wait()

        def one(g, carry):
            q, j = g // F, lax.rem(g, F)
            for n in range(blocks):
                cols = pl.ds(n * block, block)
                value = f32(cbuf[slot, g, :, cols]) * sbuf[pl.ds(pl.multiple_of((g * K + k) * sub, sub), sub), pl.ds(n, 1)]
                delta[k, q, rows(j), cols] = value.astype(jnp.bfloat16)
            return carry

        lax.fori_loop(0, R * F, one, 0, unroll=4)

    def send_first(k):
        def go(even):
            if even:
                for i in range(B - 1):
                    bb = b_peer(i)
                    for aa in range(A):
                        send(RS1, k, delta.at[k, aa * B + bb], rs1e.at[k // 2, B - 2 - i, aa], (a * B + bb, f))
            else:
                for i in range(A - 1):
                    aa = a_peer(i)
                    send(RS1, k, delta.at[k, pl.ds(aa * B, B)], rs1o.at[k // 2, A - 2 - i], (aa * B + b, f))

        by_parity(k, go)

    def stage0(k):
        @pl.when(k > 0)
        def _():
            scale_codes(k)

        send_first(k)

        @pl.when(k == 0)
        def _():
            for copy in state_in:
                copy.start()

        @pl.when(k + 2 < K)
        def _():
            for copy in load(k + 2):
                copy.start()

    def stage1(k):
        def go(even):
            wait_bytes(recv_sem, RS1, k, amount(RS1, k, even))
            buf, count, peers = (rs1e, B - 1, A - 1) if even else (rs1o, A - 1, B - 1)
            for i in range(peers):
                q = a_peer(i) if even else b_peer(i)
                target = q * B + b if even else a * B + q

                def add(j, carry):
                    total = f32(delta[k, target, rows(j), :])
                    for s in range(count):
                        total = total + f32(buf[k // 2, s, q, rows(j), :])
                    buf[k // 2, 0, q, rows(j), :] = total.astype(jnp.bfloat16)
                    return carry

                lax.fori_loop(0, F, add, 0, unroll=4)
                dst = rs2e if even else rs2o
                send(RS2, k, buf.at[k // 2, 0, q], dst.at[k // 2, peers - 1 - i], (target, f))

        by_parity(k, go)

    def stage2(k):
        def go(even):
            wait_bytes(recv_sem, RS2, k, amount(RS2, k, even))
            one, two = (rs1e, rs2e) if even else (rs1o, rs2o)
            ones, twos = (B - 1, A - 1) if even else (A - 1, B - 1)
            q = a if even else b

            def add(j, carry):
                total = f32(delta[k, r, rows(j), :])
                for s in range(ones):
                    total = total + f32(one[k // 2, s, q, rows(j), :])
                for s in range(twos):
                    total = total + f32(two[k // 2, s, rows(j), :])
                part[k, rows(j), :] = total.astype(jnp.bfloat16)
                return carry

            lax.fori_loop(0, F, add, 0, unroll=4)

        by_parity(k, go)

        @pl.when((k == 0) & (odd_core == 0))
        def _():
            pl.semaphore_wait(barrier, F - 2)
            pl.semaphore_signal(far_sem, inc=1, device_id=partner, device_id_type=MESH)

        @pl.when((k == 0) & (odd_core == 1))
        def _():
            pl.semaphore_wait(far_sem, 1)

        def out(i, carry):
            j = f_peer(i)
            send(X1, k, part.at[k, rows(j)], got.at[k, rows(f)], (r, j))
            return carry

        lax.fori_loop(0, F - 1, out, 0)
        got[k, rows(f), :] = part[k, rows(f), :]

    def stage3(k):
        @pl.when(k == 0)
        def _():
            for copy in state_in:
                copy.wait()

        wait_bytes(recv_sem, X1, k, amount(X1, k, True))
        span = pl.ds(pl.multiple_of(k * sub, sub), sub)

        def update(j, carry):
            cols = pl.ds(pl.multiple_of(j * width, width), width)
            mean = f32(got[k, rows(j), :]) * (1.0 / R)
            m = momentum_factor * new_momentum[span, cols] + mean
            p = new_master[span, cols] - outer_rate * (mean + momentum_factor * m)
            new_momentum[span, cols] = m
            new_master[span, cols] = p
            wsend[k, rows(j), :] = p.astype(jnp.bfloat16)
            return carry

        lax.fori_loop(0, F, update, 0, unroll=4)

        def out(i, carry):
            j = f_peer(i)
            send(X2, k, wsend.at[k, rows(j)], weights.at[r * F + f, k], (r, j))
            return carry

        lax.fori_loop(0, F - 1, out, 0)
        weights[r * F + f, k, :, :] = wsend[k, rows(f), :]

    def stage4(k):
        wait_bytes(recv_sem, X2, k, amount(X2, k, True))

        def go(even):
            here = weights.at[pl.ds(r * F, F), k]
            for i in range(B - 1 if even else A - 1):
                target = a * B + b_peer(i) if even else a_peer(i) * B + b
                send(AG1, k, here, here, (target, f))

        by_parity(k, go)

    def stage5(k):
        def go(even):
            wait_bytes(recv_sem, AG1, k, amount(AG1, k, even))
            if even:
                here = weights.at[pl.ds(a * B * F, B * F), k]
                for i in range(A - 1):
                    send(AG2, k, here, here, (a_peer(i) * B + b, f))
            else:
                for i in range(B - 1):
                    for aa in range(A):
                        here = weights.at[pl.ds((aa * B + b) * F, F), k]
                        send(AG2, k, here, here, (a * B + b_peer(i), f))

        by_parity(k, go)

    def stage6(k):
        def go(even):
            for stage in range(5):
                wait_bytes(send_sem, stage, k, amount(stage, k, even))
            wait_bytes(recv_sem, AG2, k, amount(AG2, k, even))
            wait_bytes(send_sem, AG2, k, amount(AG2, k, even))

        by_parity(k, go)

    stages = (stage0, stage1, stage2, stage3, stage4, stage5, stage6)

    def step(t, carry):
        for lag, stage in zip(LAGS, stages):
            k = t - lag

            @pl.when((k >= 0) & (k < K))
            def _():
                stage(k)

        return carry

    scale_codes(0)

    @pl.when(odd_core == 1)
    def _():
        pl.semaphore_wait(barrier, 2 * (A + B - 2) + 1)
        pl.semaphore_signal(near_sem, inc=1, device_id=partner, device_id_type=MESH)

    @pl.when(odd_core == 0)
    def _():
        pl.semaphore_wait(near_sem, 1)

    lax.fori_loop(0, K + LAGS[-1], step, 0)


def put(sources, targets, sem):
    copies = [
        pltpu.make_async_copy(source, target, sem.at[n]) for n, (source, target) in enumerate(zip(sources, targets))
    ]
    for copy in copies:
        copy.start()
    for copy in copies:
        copy.wait()


def solution(mesh):
    R, F = mesh.shape["replica"], mesh.shape["fsdp"]
    B = 2
    A = R // B

    def local(codes, scales, master, momentum):
        total_rows, width = codes.shape[1:]
        blocks = scales.shape[1]
        own = total_rows // (R * F)
        sub = 16 if own % 16 == 0 else own
        K = own // sub
        FS = F * sub
        even, odd = (K + 1) // 2, max(1, K // 2)
        codes = codes.reshape(R * F, K, sub, width)
        lines = max(8, blocks)
        any_spec = pl.BlockSpec(memory_space=pl.ANY)
        hbm_spec = pl.BlockSpec(memory_space=pltpu.HBM)
        bf16 = jnp.bfloat16
        state, layout = master.shape, (R * F, K, sub, width)
        results = pl.pallas_call(
            functools.partial(kernel, (A, B, F, K, sub, width, blocks)),
            out_shape=(
                pltpu.VMEM(state, jnp.float32),
                pltpu.VMEM(state, jnp.float32),
                pltpu.VMEM(layout, bf16),
            ),
            in_specs=[hbm_spec] * 4,
            out_specs=(pl.BlockSpec(memory_space=pltpu.VMEM),) * 3,
            scratch_shapes=[
                pltpu.VMEM((K, R, FS, width), bf16),
                pltpu.VMEM((even, B - 1, A, FS, width), bf16),
                pltpu.VMEM((odd, A - 1, B, FS, width), bf16),
                pltpu.VMEM((even, A - 1, FS, width), bf16),
                pltpu.VMEM((odd, B - 1, FS, width), bf16),
                pltpu.VMEM((K, FS, width), bf16),
                pltpu.VMEM((K, FS, width), bf16),
                pltpu.VMEM((K, FS, width), bf16),
                pltpu.VMEM((2, R * F, sub, width), jnp.int32),
                pltpu.VMEM((lines, total_rows), jnp.float32),
                pltpu.VMEM((total_rows, lines), jnp.float32),
                pltpu.SemaphoreType.DMA((6, K)),
                pltpu.SemaphoreType.DMA((6, K)),
                pltpu.SemaphoreType.DMA((2, R)),
                pltpu.SemaphoreType.DMA((3,)),
                pltpu.SemaphoreType.REGULAR,
                pltpu.SemaphoreType.REGULAR,
            ],
            compiler_params=pltpu.CompilerParams(
                collective_id=0, has_side_effects=True, vmem_limit_bytes=36 * 1024 * 1024
            ),
        )(codes, scales, master, momentum)
        new_master, new_momentum, weights = pl.pallas_call(
            lambda *refs: put(refs[:3], refs[3:6], refs[6]),
            out_shape=(
                jax.ShapeDtypeStruct(state, jnp.float32),
                jax.ShapeDtypeStruct(state, jnp.float32),
                jax.ShapeDtypeStruct(layout, bf16),
            ),
            in_specs=[any_spec] * 3,
            out_specs=(hbm_spec,) * 3,
            scratch_shapes=[pltpu.SemaphoreType.DMA((3,))],
            compiler_params=pltpu.CompilerParams(vmem_limit_bytes=1024 * 1024),
        )(*results)
        return (new_master, new_momentum, weights.reshape(total_rows, width))

    return jax.shard_map(
        local,
        mesh=mesh,
        in_specs=(
            P("replica", None, "fsdp"),
            P("replica", "fsdp", None),
            P(("replica", "fsdp"), None),
            P(("replica", "fsdp"), None),
        ),
        out_specs=(P(("replica", "fsdp"), None), P(("replica", "fsdp"), None), P(None, "fsdp")),
        check_vma=False,
    )
```

```python
import functools

import jax
import jax.numpy as jnp
from jax import lax
from jax.experimental import pallas as pl
from jax.experimental.pallas import tpu as pltpu
from jax.sharding import PartitionSpec as P

MESH = pl.DeviceIdType.MESH

outer_rate = 0.7
momentum_factor = 0.9

LAGS = (0, 3, 6, 8, 10, 13, 16)
RS1, RS2, X1, X2, AG1, AG2 = range(6)


def kernel(cfg, codes, scales, master, momentum, new_master, new_momentum, weights,
           delta, rs1e, rs1o, rs2e, rs2o, part, got, wsend, cbuf, flat, sbuf,
           send_sem, recv_sem, in_sem, scale_sem, state_sem, near_sem, far_sem):
    A, B, F, K, sub, width, blocks = cfg
    R, block, own = A * B, width // blocks, K * sub
    r, f = lax.axis_index("replica"), lax.axis_index("fsdp")
    a, b = r // B, lax.rem(r, B)
    odd_core = lax.rem(f, 2)
    partner = (r, f + 1 - 2 * odd_core)

    def a_peer(i):
        return lax.rem(a + 1 + i, A)

    def b_peer(i):
        return lax.rem(b + 1 + i, B)

    def f_peer(i):
        return lax.rem(f + 1 + i, F)

    barrier = pltpu.get_barrier_semaphore()
    near = f - odd_core + 1
    for i in range(A - 1):
        pl.semaphore_signal(barrier, inc=1, device_id=(a_peer(i) * B + b, near), device_id_type=MESH)
    for i in range(B - 1):
        pl.semaphore_signal(barrier, inc=1, device_id=(a * B + b_peer(i), near), device_id_type=MESH)

    @pl.when(odd_core == 0)
    def _():
        pl.semaphore_signal(barrier, inc=1, device_id=partner, device_id_type=MESH)

    def offsets(even, p):
        if even:
            return lax.rem(1 + lax.rem(p, A), A), lax.rem(1 + p // A, B)
        return lax.rem(1 + p // B, A), lax.rem(1 + lax.rem(p, B), B)

    def at(da, db):
        return lax.rem(a + da, A) * B + lax.rem(b + db, B)

    def load(k, q):
        slot, group = lax.rem(k, 2), pl.ds(q * F, F)
        return pltpu.make_async_copy(codes.at[group, k], cbuf.at[slot, group], in_sem.at[slot, q])

    def scales_in(q):
        group = pl.ds(q * F * own, F * own)
        return pltpu.make_async_copy(scales.at[0, :, group], flat.at[pl.ds(0, blocks), group], scale_sem.at[q])

    first = tuple(
        (k, p, ((1 + p % A) % A, (1 + p // A) % B) if k == 0 else ((1 + p // B) % A, (1 + p % B) % B))
        for p in range(R) for k in range(min(2, K))
    )
    seen = set()
    for k, p, spot in first:
        if spot not in seen:
            seen.add(spot)
            scales_in(at(*spot)).start()
        load(k, at(*spot)).start()

    for i in range(F // 2 - 1):
        pair = lax.rem(f // 2 + 1 + i, F // 2)
        pl.semaphore_signal(barrier, inc=1, device_id=(r, 2 * pair), device_id_type=MESH)

    state_in = (
        pltpu.make_async_copy(master, new_master, state_sem.at[0]),
        pltpu.make_async_copy(momentum, new_momentum, state_sem.at[1]),
    )

    def turn(i):
        span = pl.ds(pl.multiple_of(i * 128, 128), 128)
        sbuf[span, :] = jnp.transpose(flat[:, span])

    def send(stage, k, src, dst, device):
        pltpu.make_async_remote_copy(
            src_ref=src, dst_ref=dst, send_sem=send_sem.at[stage, k], recv_sem=recv_sem.at[stage, k],
            device_id=device, device_id_type=MESH,
        ).start()

    def wait_bytes(sem, stage, k, ref):
        pltpu.make_async_copy(ref, ref, sem.at[stage, k]).wait()

    def rows(j):
        return pl.ds(pl.multiple_of(j * sub, sub), sub)

    def f32(x):
        return x.astype(jnp.float32)

    def amount(stage, k, even):
        if stage == RS1:
            return rs1e.at[k // 2] if even else rs1o.at[k // 2]
        if stage == RS2:
            return rs2e.at[k // 2] if even else rs2o.at[k // 2]
        if stage in (X1, X2):
            return part.at[k, pl.ds(0, (F - 1) * sub)]
        first, second = (B - 1, B * (A - 1)) if even else (A - 1, A * (B - 1))
        count = first if stage == AG1 else second
        return delta.at[k, pl.ds(0, count)]

    def by_parity(k, fn):
        @pl.when(lax.rem(k, 2) == 0)
        def _():
            fn(True)

        if K > 1:
            @pl.when(lax.rem(k, 2) == 1)
            def _():
                fn(False)

    def turn_scales(k, q):
        each, tiles = (F, own // 128) if own % 128 == 0 else (F * own // 128, 1)
        part = k * sub // 128 if own % 128 == 0 else 0

        def some(j, carry):
            turn((q * each + j) * tiles + part)
            return carry

        lax.fori_loop(0, each, some, 0, unroll=8)

    def scale_piece(k, q):
        slot = lax.rem(k, 2)
        load(k, q).wait()

        def one(j, carry):
            g = q * F + j
            for n in range(blocks):
                cols = pl.ds(n * block, block)
                value = f32(cbuf[slot, g, :, cols]) * sbuf[rows(g * K + k), pl.ds(n, 1)]
                delta[k, q, rows(j), cols] = value.astype(jnp.bfloat16)
            return carry

        lax.fori_loop(0, F, one, 0, unroll=4)

    def send_even(k, p, q):
        i, aa = p // A, q // B
        send(RS1, k, delta.at[k, q], rs1e.at[k // 2, B - 2 - i, aa], (a * B + lax.rem(q, B), f))

    def send_odd(k, p, q):
        i, bb = p // B, lax.rem(q, B)
        send(RS1, k, delta.at[k, q], rs1o.at[k // 2, A - 2 - i, bb], ((q // B) * B + b, f))

    def refill(k):
        @pl.when(k + 2 < K)
        def _():
            for q in range(R):
                load(k + 2, q).start()

    def begin():
        seen = set()
        for n, (k, p, spot) in enumerate(first):
            q = at(*spot)
            if spot not in seen:
                seen.add(spot)
                scales_in(q).wait()
                turn_scales(0, q)
            scale_piece(k, q)
            if n == 0:
                @pl.when(odd_core == 1)
                def _():
                    pl.semaphore_wait(barrier, 2 * (A + B - 2) + 1)
                    pl.semaphore_signal(near_sem, inc=1, device_id=partner, device_id_type=MESH)

                @pl.when(odd_core == 0)
                def _():
                    pl.semaphore_wait(near_sem, 1)

            if k == 0 and p < A * (B - 1):
                send_even(k, p, q)
            if k == 1 and p < B * (A - 1):
                send_odd(k, p, q)
        for k in range(min(2, K)):
            refill(k)
        for copy in state_in:
            copy.start()

    def stage0(k):
        def piece(even, p, carry):
            q = at(*offsets(even, p))
            if own % 128 == 0:
                @pl.when(lax.rem(k, 128 // sub) == 0)
                def _():
                    turn_scales(k, q)

            scale_piece(k, q)

            @pl.when(p < (A * (B - 1) if even else B * (A - 1)))
            def _():
                (send_even if even else send_odd)(k, p, q)

            return carry

        by_parity(k, lambda even: lax.fori_loop(0, R, functools.partial(piece, even), 0))
        refill(k)

    def stage1(k):
        def go(even):
            wait_bytes(recv_sem, RS1, k, amount(RS1, k, even))
            buf, count, peers = (rs1e, B - 1, A - 1) if even else (rs1o, A - 1, B - 1)
            for i in range(peers):
                q = a_peer(i) if even else b_peer(i)
                target = q * B + b if even else a * B + q

                def add(j, carry):
                    total = f32(delta[k, target, rows(j), :])
                    for s in range(count):
                        total = total + f32(buf[k // 2, s, q, rows(j), :])
                    buf[k // 2, 0, q, rows(j), :] = total.astype(jnp.bfloat16)
                    return carry

                lax.fori_loop(0, F, add, 0, unroll=4)
                dst = rs2e if even else rs2o
                send(RS2, k, buf.at[k // 2, 0, q], dst.at[k // 2, peers - 1 - i], (target, f))

        by_parity(k, go)

    def stage2(k):
        def go(even):
            wait_bytes(recv_sem, RS2, k, amount(RS2, k, even))
            one, two = (rs1e, rs2e) if even else (rs1o, rs2o)
            ones, twos = (B - 1, A - 1) if even else (A - 1, B - 1)
            q = a if even else b

            def add(j, carry):
                total = f32(delta[k, r, rows(j), :])
                for s in range(ones):
                    total = total + f32(one[k // 2, s, q, rows(j), :])
                for s in range(twos):
                    total = total + f32(two[k // 2, s, rows(j), :])
                part[k, rows(j), :] = total.astype(jnp.bfloat16)
                return carry

            lax.fori_loop(0, F, add, 0, unroll=4)

        by_parity(k, go)

        @pl.when((k == 0) & (odd_core == 0))
        def _():
            pl.semaphore_wait(barrier, F - 2)
            pl.semaphore_signal(far_sem, inc=1, device_id=partner, device_id_type=MESH)

        @pl.when((k == 0) & (odd_core == 1))
        def _():
            pl.semaphore_wait(far_sem, 1)

        def out(i, carry):
            j = f_peer(i)
            send(X1, k, part.at[k, rows(j)], got.at[k, rows(f)], (r, j))
            return carry

        lax.fori_loop(0, F - 1, out, 0)
        got[k, rows(f), :] = part[k, rows(f), :]

    def stage3(k):
        @pl.when(k == 0)
        def _():
            for copy in state_in:
                copy.wait()

        wait_bytes(recv_sem, X1, k, amount(X1, k, True))
        span = pl.ds(pl.multiple_of(k * sub, sub), sub)

        def update(j, carry):
            cols = pl.ds(pl.multiple_of(j * width, width), width)
            mean = f32(got[k, rows(j), :]) * (1.0 / R)
            m = momentum_factor * new_momentum[span, cols] + mean
            p = new_master[span, cols] - outer_rate * (mean + momentum_factor * m)
            new_momentum[span, cols] = m
            new_master[span, cols] = p
            wsend[k, rows(j), :] = p.astype(jnp.bfloat16)
            return carry

        lax.fori_loop(0, F, update, 0, unroll=4)

        def out(i, carry):
            j = f_peer(i)
            send(X2, k, wsend.at[k, rows(j)], weights.at[r * F + f, k], (r, j))
            return carry

        lax.fori_loop(0, F - 1, out, 0)
        weights[r * F + f, k, :, :] = wsend[k, rows(f), :]

    def stage4(k):
        wait_bytes(recv_sem, X2, k, amount(X2, k, True))

        def go(even):
            here = weights.at[pl.ds(r * F, F), k]
            for i in range(B - 1 if even else A - 1):
                target = a * B + b_peer(i) if even else a_peer(i) * B + b
                send(AG1, k, here, here, (target, f))

        by_parity(k, go)

    def stage5(k):
        def go(even):
            wait_bytes(recv_sem, AG1, k, amount(AG1, k, even))
            if even:
                here = weights.at[pl.ds(a * B * F, B * F), k]
                for i in range(A - 1):
                    send(AG2, k, here, here, (a_peer(i) * B + b, f))
            else:
                for i in range(B - 1):
                    for aa in range(A):
                        here = weights.at[pl.ds((aa * B + b) * F, F), k]
                        send(AG2, k, here, here, (a * B + b_peer(i), f))

        by_parity(k, go)

    def stage6(k):
        def go(even):
            for stage in range(5):
                wait_bytes(send_sem, stage, k, amount(stage, k, even))
            wait_bytes(recv_sem, AG2, k, amount(AG2, k, even))
            wait_bytes(send_sem, AG2, k, amount(AG2, k, even))

        by_parity(k, go)

    stages = (stage0, stage1, stage2, stage3, stage4, stage5, stage6)

    def step(t, carry):
        for lag, stage in zip(LAGS, stages):
            k = t - lag

            @pl.when((k >= (min(2, K) if stage is stage0 else 0)) & (k < K))
            def _():
                stage(k)

        return carry

    begin()
    lax.fori_loop(0, K + LAGS[-1], step, 0)


def put(sources, targets, sem):
    copies = [
        pltpu.make_async_copy(source, target, sem.at[n]) for n, (source, target) in enumerate(zip(sources, targets))
    ]
    for copy in copies:
        copy.start()
    for copy in copies:
        copy.wait()


def solution(mesh):
    R, F = mesh.shape["replica"], mesh.shape["fsdp"]
    B = 2
    A = R // B

    def local(codes, scales, master, momentum):
        total_rows, width = codes.shape[1:]
        blocks = scales.shape[1]
        own = total_rows // (R * F)
        sub = 16 if own % 16 == 0 else own
        K = own // sub
        FS = F * sub
        even, odd = (K + 1) // 2, max(1, K // 2)
        codes = codes.reshape(R * F, K, sub, width)
        lines = max(8, blocks)
        any_spec = pl.BlockSpec(memory_space=pl.ANY)
        hbm_spec = pl.BlockSpec(memory_space=pltpu.HBM)
        bf16 = jnp.bfloat16
        state, layout = master.shape, (R * F, K, sub, width)
        results = pl.pallas_call(
            functools.partial(kernel, (A, B, F, K, sub, width, blocks)),
            out_shape=(
                pltpu.VMEM(state, jnp.float32),
                pltpu.VMEM(state, jnp.float32),
                pltpu.VMEM(layout, bf16),
            ),
            in_specs=[hbm_spec] * 4,
            out_specs=(pl.BlockSpec(memory_space=pltpu.VMEM),) * 3,
            scratch_shapes=[
                pltpu.VMEM((K, R, FS, width), bf16),
                pltpu.VMEM((even, B - 1, A, FS, width), bf16),
                pltpu.VMEM((odd, A - 1, B, FS, width), bf16),
                pltpu.VMEM((even, A - 1, FS, width), bf16),
                pltpu.VMEM((odd, B - 1, FS, width), bf16),
                pltpu.VMEM((K, FS, width), bf16),
                pltpu.VMEM((K, FS, width), bf16),
                pltpu.VMEM((K, FS, width), bf16),
                pltpu.VMEM((2, R * F, sub, width), jnp.int32),
                pltpu.VMEM((lines, total_rows), jnp.float32),
                pltpu.VMEM((total_rows, lines), jnp.float32),
                pltpu.SemaphoreType.DMA((6, K)),
                pltpu.SemaphoreType.DMA((6, K)),
                pltpu.SemaphoreType.DMA((2, R)),
                pltpu.SemaphoreType.DMA((R,)),
                pltpu.SemaphoreType.DMA((2,)),
                pltpu.SemaphoreType.REGULAR,
                pltpu.SemaphoreType.REGULAR,
            ],
            compiler_params=pltpu.CompilerParams(
                collective_id=0, has_side_effects=True, vmem_limit_bytes=46 * 1024 * 1024
            ),
        )(codes, scales, master, momentum)
        new_master, new_momentum, weights = pl.pallas_call(
            lambda *refs: put(refs[:3], refs[3:6], refs[6]),
            out_shape=(
                jax.ShapeDtypeStruct(state, jnp.float32),
                jax.ShapeDtypeStruct(state, jnp.float32),
                jax.ShapeDtypeStruct(layout, bf16),
            ),
            in_specs=[any_spec] * 3,
            out_specs=(hbm_spec,) * 3,
            scratch_shapes=[pltpu.SemaphoreType.DMA((3,))],
            compiler_params=pltpu.CompilerParams(vmem_limit_bytes=1024 * 1024),
        )(*results)
        return (new_master, new_momentum, weights.reshape(total_rows, width))

    return jax.shard_map(
        local,
        mesh=mesh,
        in_specs=(
            P("replica", None, "fsdp"),
            P("replica", "fsdp", None),
            P(("replica", "fsdp"), None),
            P(("replica", "fsdp"), None),
        ),
        out_specs=(P(("replica", "fsdp"), None), P(("replica", "fsdp"), None), P(None, "fsdp")),
        check_vma=False,
    )
```

```python
import functools

import jax
import jax.numpy as jnp
from jax import lax
from jax.experimental import pallas as pl
from jax.experimental.pallas import tpu as pltpu
from jax.sharding import PartitionSpec as P

MESH = pl.DeviceIdType.MESH

outer_rate = 0.7
momentum_factor = 0.9

LAGS = (0, 3, 6, 8, 10, 13, 13, 16)
EARLY = (8, 10, 16)
LONG = 0
TAIL = 10
RS1, RS2, X1, X2, AG1, AG2 = range(6)


def spread(even, A, B, F, a, b):
    if even:
        return [(pl.ds(a * B * F, B * F), i, pl.ds((A - 2 - i) * B * F, B * F)) for i in range(A - 1)]
    return [
        (pl.ds((aa * B + b) * F, F), i, pl.ds(((B - 2 - i) * A + aa) * F, F)) for i in range(B - 1) for aa in range(A)
    ]


def gathered(even, A, B, F, a, b):
    if even:
        return [(pl.ds(i * B * F, B * F), pl.ds(lax.rem(a + 1 + i, A) * B * F, B * F)) for i in range(A - 1)]
    return [
        (pl.ds((i * A + aa) * F, F), pl.ds((aa * B + lax.rem(b + 1 + i, B)) * F, F)) for i in range(B - 1) for aa in range(A)
    ]


def kernel(cfg, codes, scales, master, momentum, new_master, new_momentum, weights,
           delta, rs1e, rs1o, rs2e, rs2o, part, got, wsend, cbuf, flat, sbuf,
           send_sem, recv_sem, in_sem, scale_sem, state_sem, near_sem, far_sem):
    A, B, F, K, sub, width, blocks, late = cfg
    R, block, own = A * B, width // blocks, K * sub
    r, f = lax.axis_index("replica"), lax.axis_index("fsdp")
    a, b = r // B, lax.rem(r, B)
    odd_core = lax.rem(f, 2)
    held = jnp.where(odd_core == LONG, late[1], late[0])
    spread_out = jnp.where(odd_core == LONG, late[2], late[0])
    partner = (r, f + 1 - 2 * odd_core)

    def a_peer(i):
        return lax.rem(a + 1 + i, A)

    def b_peer(i):
        return lax.rem(b + 1 + i, B)

    def f_peer(i):
        return lax.rem(f + 1 + i, F)

    barrier = pltpu.get_barrier_semaphore()
    near = f - odd_core + 1
    for i in range(A - 1):
        pl.semaphore_signal(barrier, inc=1, device_id=(a_peer(i) * B + b, near), device_id_type=MESH)
    for i in range(B - 1):
        pl.semaphore_signal(barrier, inc=1, device_id=(a * B + b_peer(i), near), device_id_type=MESH)

    @pl.when(odd_core == 0)
    def _():
        pl.semaphore_signal(barrier, inc=1, device_id=partner, device_id_type=MESH)

    def offsets(even, p):
        if even:
            return lax.rem(1 + lax.rem(p, A), A), lax.rem(1 + p // A, B)
        return lax.rem(1 + p // B, A), lax.rem(1 + lax.rem(p, B), B)

    def at(da, db):
        return lax.rem(a + da, A) * B + lax.rem(b + db, B)

    def load(k, q):
        slot, group = lax.rem(k, 2), pl.ds(q * F, F)
        return pltpu.make_async_copy(codes.at[group, k], cbuf.at[slot, group], in_sem.at[slot, q])

    def scales_in(q):
        group = pl.ds(q * F * own, F * own)
        return pltpu.make_async_copy(scales.at[0, :, group], flat.at[pl.ds(0, blocks), group], scale_sem.at[q])

    first = tuple(
        (k, p, ((1 + p % A) % A, (1 + p // A) % B) if k == 0 else ((1 + p // B) % A, (1 + p % B) % B))
        for p in range(R) for k in range(min(2, K))
    )
    seen = set()
    for k, p, spot in first:
        if spot not in seen:
            seen.add(spot)
            scales_in(at(*spot)).start()
        load(k, at(*spot)).start()

    for i in range(F // 2 - 1):
        pair = lax.rem(f // 2 + 1 + i, F // 2)
        pl.semaphore_signal(barrier, inc=1, device_id=(r, 2 * pair), device_id_type=MESH)

    state_in = (
        pltpu.make_async_copy(master, new_master, state_sem.at[0]),
        pltpu.make_async_copy(momentum, new_momentum, state_sem.at[1]),
    )

    def turn(i):
        span = pl.ds(pl.multiple_of(i * 128, 128), 128)
        sbuf[span, :] = jnp.transpose(flat[:, span])

    def send(stage, k, src, dst, device):
        pltpu.make_async_remote_copy(
            src_ref=src, dst_ref=dst, send_sem=send_sem.at[stage, k], recv_sem=recv_sem.at[stage, k],
            device_id=device, device_id_type=MESH,
        ).start()

    def wait_bytes(sem, stage, k, ref):
        pltpu.make_async_copy(ref, ref, sem.at[stage, k]).wait()

    def rows(j):
        return pl.ds(pl.multiple_of(j * sub, sub), sub)

    def f32(x):
        return x.astype(jnp.float32)

    def amount(stage, k, even):
        if stage == RS1:
            return rs1e.at[k // 2] if even else rs1o.at[k // 2]
        if stage == RS2:
            return rs2e.at[k // 2] if even else rs2o.at[k // 2]
        if stage in (X1, X2):
            return part.at[k, pl.ds(0, (F - 1) * sub)]
        first, second = (B - 1, B * (A - 1)) if even else (A - 1, A * (B - 1))
        count = first if stage == AG1 else second
        return delta.at[k, pl.ds(0, count)]

    def by_parity(k, fn):
        @pl.when(lax.rem(k, 2) == 0)
        def _():
            fn(True)

        if K > 1:
            @pl.when(lax.rem(k, 2) == 1)
            def _():
                fn(False)

    def turn_scales(k, q):
        each, tiles = (F, own // 128) if own % 128 == 0 else (F * own // 128, 1)
        part = k * sub // 128 if own % 128 == 0 else 0

        def some(j, carry):
            turn((q * each + j) * tiles + part)
            return carry

        lax.fori_loop(0, each, some, 0, unroll=8)

    def scale_piece(k, q):
        slot = lax.rem(k, 2)
        load(k, q).wait()

        def one(j, carry):
            g = q * F + j
            for n in range(blocks):
                cols = pl.ds(n * block, block)
                value = f32(cbuf[slot, g, :, cols]) * sbuf[rows(g * K + k), pl.ds(n, 1)]
                delta[k, q, rows(j), cols] = value.astype(jnp.bfloat16)
            return carry

        lax.fori_loop(0, F, one, 0, unroll=4)

    def send_even(k, p, q):
        i, aa = p // A, q // B
        send(RS1, k, delta.at[k, q], rs1e.at[k // 2, B - 2 - i, aa], (a * B + lax.rem(q, B), f))

    def send_odd(k, p, q):
        i, bb = p // B, lax.rem(q, B)
        send(RS1, k, delta.at[k, q], rs1o.at[k // 2, A - 2 - i, bb], ((q // B) * B + b, f))

    def refill(k):
        @pl.when(k + 2 < K)
        def _():
            for q in range(R):
                load(k + 2, q).start()

    def begin():
        seen = set()
        for n, (k, p, spot) in enumerate(first):
            q = at(*spot)
            if spot not in seen:
                seen.add(spot)
                scales_in(q).wait()
                turn_scales(0, q)
            scale_piece(k, q)
            if n == 0:
                @pl.when(odd_core == 1)
                def _():
                    pl.semaphore_wait(barrier, 2 * (A + B - 2) + 1)
                    pl.semaphore_signal(near_sem, inc=1, device_id=partner, device_id_type=MESH)

                @pl.when(odd_core == 0)
                def _():
                    pl.semaphore_wait(near_sem, 1)

            if k == 0 and p < A * (B - 1):
                send_even(k, p, q)
            if k == 1 and p < B * (A - 1):
                send_odd(k, p, q)
        for k in range(min(2, K)):
            refill(k)
        for copy in state_in:
            copy.start()

    def stage0(k):
        def piece(even, p, carry):
            q = at(*offsets(even, p))
            if own % 128 == 0:
                @pl.when(lax.rem(k, 128 // sub) == 0)
                def _():
                    turn_scales(k, q)

            scale_piece(k, q)

            @pl.when(p < (A * (B - 1) if even else B * (A - 1)))
            def _():
                (send_even if even else send_odd)(k, p, q)

            return carry

        by_parity(k, lambda even: lax.fori_loop(0, R, functools.partial(piece, even), 0))
        refill(k)

    def stage1(k):
        def go(even):
            wait_bytes(recv_sem, RS1, k, amount(RS1, k, even))
            buf, count, peers = (rs1e, B - 1, A - 1) if even else (rs1o, A - 1, B - 1)
            for i in range(peers):
                q = a_peer(i) if even else b_peer(i)
                target = q * B + b if even else a * B + q

                def add(j, carry):
                    total = f32(delta[k, target, rows(j), :])
                    for s in range(count):
                        total = total + f32(buf[k // 2, s, q, rows(j), :])
                    buf[k // 2, 0, q, rows(j), :] = total.astype(jnp.bfloat16)
                    return carry

                lax.fori_loop(0, F, add, 0, unroll=4)
                dst = rs2e if even else rs2o
                send(RS2, k, buf.at[k // 2, 0, q], dst.at[k // 2, peers - 1 - i], (target, f))

        by_parity(k, go)

    def stage2(k):
        def go(even):
            wait_bytes(recv_sem, RS2, k, amount(RS2, k, even))
            one, two = (rs1e, rs2e) if even else (rs1o, rs2o)
            ones, twos = (B - 1, A - 1) if even else (A - 1, B - 1)
            q = a if even else b

            def add(j, carry):
                total = f32(delta[k, r, rows(j), :])
                for s in range(ones):
                    total = total + f32(one[k // 2, s, q, rows(j), :])
                for s in range(twos):
                    total = total + f32(two[k // 2, s, rows(j), :])
                part[k, rows(j), :] = total.astype(jnp.bfloat16)
                return carry

            lax.fori_loop(0, F, add, 0, unroll=4)

        by_parity(k, go)

        @pl.when((k == 0) & (odd_core == 0))
        def _():
            pl.semaphore_wait(barrier, F - 2)
            pl.semaphore_signal(far_sem, inc=1, device_id=partner, device_id_type=MESH)

        @pl.when((k == 0) & (odd_core == 1))
        def _():
            pl.semaphore_wait(far_sem, 1)

        def out(i, carry):
            j = f_peer(i)
            send(X1, k, part.at[k, rows(j)], got.at[k, rows(f)], (r, j))
            return carry

        lax.fori_loop(0, F - 1, out, 0)
        got[k, rows(f), :] = part[k, rows(f), :]

    def stage3(k):
        @pl.when(k == 0)
        def _():
            for copy in state_in:
                copy.wait()

        wait_bytes(recv_sem, X1, k, amount(X1, k, True))
        span = pl.ds(pl.multiple_of(k * sub, sub), sub)

        def update(j, carry):
            cols = pl.ds(pl.multiple_of(j * width, width), width)
            mean = f32(got[k, rows(j), :]) * (1.0 / R)
            m = momentum_factor * new_momentum[span, cols] + mean
            p = new_master[span, cols] - outer_rate * (mean + momentum_factor * m)
            new_momentum[span, cols] = m
            new_master[span, cols] = p
            wsend[k, rows(j), :] = p.astype(jnp.bfloat16)
            return carry

        lax.fori_loop(0, F, update, 0, unroll=4)

        def out(i, carry):
            j = f_peer(i)
            send(X2, k, wsend.at[k, rows(j)], weights.at[r * F + f, k], (r, j))
            return carry

        lax.fori_loop(0, F - 1, out, 0)
        weights[r * F + f, k, :, :] = wsend[k, rows(f), :]

    def stage4(k):
        wait_bytes(recv_sem, X2, k, amount(X2, k, True))

        def go(even):
            here = weights.at[pl.ds(r * F, F), k]
            for i in range(B - 1 if even else A - 1):
                target = a * B + b_peer(i) if even else a_peer(i) * B + b
                send(AG1, k, here, here, (target, f))

        by_parity(k, go)

    def stage5(k):
        by_parity(k, lambda even: wait_bytes(recv_sem, AG1, k, amount(AG1, k, even)))

    def gather_on(k):
        def go(even):
            for source, i, spot in spread(even, A, B, F, a, b):
                here = weights.at[source, k]
                send(AG2, k, here, here, ((a_peer(i) * B + b, f) if even else (a * B + b_peer(i), f)))

        by_parity(k, go)

    def gather_end(k):
        def go(even):
            wait_bytes(recv_sem, AG2, k, amount(AG2, k, even))
            wait_bytes(send_sem, AG2, k, amount(AG2, k, even))

        by_parity(k, go)

    def stage6(k):
        pl.when((k < spread_out) | ((k > K - 1 + TAIL - LAGS[6]) & (k < held)))(lambda: gather_on(k))

    def stage7(k):
        def go(even):
            for stage in range(5):
                wait_bytes(send_sem, stage, k, amount(stage, k, even))

        by_parity(k, go)
        pl.when(k < spread_out)(lambda: gather_end(k))

    stages = (stage0, stage1, stage2, stage3, stage4, stage5, stage6, stage7)

    def loop(fn, end):
        def one(k, carry):
            fn(k)
            return carry

        lax.fori_loop(spread_out, end, one, 0)

    def step(t, carry):
        for lag, stage in zip(LAGS, stages):
            k = t - lag

            @pl.when((k >= (min(2, K) if stage is stage0 else 0)) & (k < K))
            def _():
                stage(k)

        @pl.when(t == K - 1 + TAIL)
        def _():
            loop(gather_on, jnp.minimum(held, max(0, K + TAIL - LAGS[6])))

        return carry

    begin()
    lax.fori_loop(0, K + LAGS[-1], step, 0)
    loop(gather_end, held)


def position(cfg):
    A, B, F, K, late = cfg
    r, f = lax.axis_index("replica"), lax.axis_index("fsdp")
    return r // B, lax.rem(r, B), f, jnp.where(lax.rem(f, 2) == LONG, late[1], late[0])


def gather_late(cfg, weights, token, tail, send_sem, recv_sem):
    A, B, F, K, late = cfg
    a, b, f, held = position(cfg)
    barrier = pltpu.get_barrier_semaphore()
    peers = [(lax.rem(a + 1 + i, A) * B + b, f) for i in range(A - 1)]
    peers += [(a * B + lax.rem(b + 1 + i, B), f) for i in range(B - 1)]
    for peer in peers:
        pl.semaphore_signal(barrier, inc=1, device_id=peer, device_id_type=MESH)
    pl.semaphore_wait(barrier, A + B - 2)

    def each(fn):
        def one(k, carry):
            for even in (True, False):
                @pl.when(lax.rem(k, 2) == (0 if even else 1))
                def _():
                    fn(k, even)

            return carry

        lax.fori_loop(held, K, one, 0)

    def start(k, even):
        for source, i, slot in spread(even, A, B, F, a, b):
            pltpu.make_async_remote_copy(
                src_ref=weights.at[source, k], dst_ref=tail.at[k - min(late[:2]), slot],
                send_sem=send_sem.at[k], recv_sem=recv_sem.at[k],
                device_id=peers[i] if even else peers[A - 1 + i], device_id_type=MESH,
            ).start()

    def finish(k, even):
        moved = tail.at[k - min(late[:2]), pl.ds(0, ((A - 1) * B if even else A * (B - 1)) * F)]
        pltpu.make_async_copy(moved, moved, recv_sem.at[k]).wait()
        pltpu.make_async_copy(moved, moved, send_sem.at[k]).wait()

    each(start)
    each(finish)


def write_early(cfg, master, momentum, weights, new_master, new_momentum, written, token, state_sem, sem, late_sem):
    A, B, F, K, late = cfg
    a, b, f, held = position(cfg)
    copies = [
        pltpu.make_async_copy(master, new_master, state_sem.at[0]),
        pltpu.make_async_copy(momentum, new_momentum, state_sem.at[1]),
    ]
    for copy in copies:
        copy.start()

    def each(act):
        for k in range(K):
            if k < max(late[:2]):
                def whole(k=k):
                    act(pltpu.make_async_copy(weights.at[:, k], written.at[:, k], sem.at[k]))

                pl.when(k < held)(whole)
            if k >= min(late[:2]):
                def mine(k=k):
                    group = [pl.ds(a * B * F, B * F)] if k % 2 == 0 else [pl.ds((aa * B + b) * F, F) for aa in range(A)]
                    for n, blocks in enumerate(group):
                        act(pltpu.make_async_copy(weights.at[blocks, k], written.at[blocks, k], late_sem.at[k, n]))

                pl.when(k >= held)(mine)

    each(lambda copy: copy.start())
    token[...] = jnp.zeros_like(token)
    each(lambda copy: copy.wait())
    for copy in copies:
        copy.wait()


def write_late(cfg, written, tail, weights, sem):
    A, B, F, K, late = cfg
    a, b, f, held = position(cfg)

    def each(act):
        for k in range(min(late[:2]), K):
            def piece(k=k):
                for n, (slot, blocks) in enumerate(gathered(k % 2 == 0, A, B, F, a, b)):
                    act(pltpu.make_async_copy(tail.at[k - min(late[:2]), slot], weights.at[blocks, k], sem.at[k, n]))

            pl.when(k >= held)(piece)

    each(lambda copy: copy.start())
    each(lambda copy: copy.wait())


def solution(mesh):
    R, F = mesh.shape["replica"], mesh.shape["fsdp"]
    B = 2
    A = R // B

    def local(codes, scales, master, momentum):
        total_rows, width = codes.shape[1:]
        blocks = scales.shape[1]
        own = total_rows // (R * F)
        sub = 16 if own % 16 == 0 else own
        K = own // sub
        FS = F * sub
        even, odd = (K + 1) // 2, max(1, K // 2)
        codes = codes.reshape(R * F, K, sub, width)
        lines = max(8, blocks)
        any_spec = pl.BlockSpec(memory_space=pl.ANY)
        hbm_spec = pl.BlockSpec(memory_space=pltpu.HBM)
        bf16 = jnp.bfloat16
        late = (K * EARLY[0] // 16, K * EARLY[2] // 16, K * EARLY[1] // 16)
        state, layout = master.shape, (R * F, K, sub, width)
        new_master, new_momentum, gathered_early = pl.pallas_call(
            functools.partial(kernel, (A, B, F, K, sub, width, blocks, late)),
            out_shape=(
                pltpu.VMEM(state, jnp.float32),
                pltpu.VMEM(state, jnp.float32),
                pltpu.VMEM(layout, bf16),
            ),
            in_specs=[hbm_spec] * 4,
            out_specs=(pl.BlockSpec(memory_space=pltpu.VMEM),) * 3,
            scratch_shapes=[
                pltpu.VMEM((K, R, FS, width), bf16),
                pltpu.VMEM((even, B - 1, A, FS, width), bf16),
                pltpu.VMEM((odd, A - 1, B, FS, width), bf16),
                pltpu.VMEM((even, A - 1, FS, width), bf16),
                pltpu.VMEM((odd, B - 1, FS, width), bf16),
                pltpu.VMEM((K, FS, width), bf16),
                pltpu.VMEM((K, FS, width), bf16),
                pltpu.VMEM((K, FS, width), bf16),
                pltpu.VMEM((2, R * F, sub, width), jnp.int32),
                pltpu.VMEM((lines, total_rows), jnp.float32),
                pltpu.VMEM((total_rows, lines), jnp.float32),
                pltpu.SemaphoreType.DMA((6, K)),
                pltpu.SemaphoreType.DMA((6, K)),
                pltpu.SemaphoreType.DMA((2, R)),
                pltpu.SemaphoreType.DMA((R,)),
                pltpu.SemaphoreType.DMA((2,)),
                pltpu.SemaphoreType.REGULAR,
                pltpu.SemaphoreType.REGULAR,
            ],
            compiler_params=pltpu.CompilerParams(
                collective_id=0, has_side_effects=True, vmem_limit_bytes=46 * 1024 * 1024
            ),
        )(codes, scales, master, momentum)
        small = dict(vmem_limit_bytes=1024 * 1024)
        plan = (A, B, F, K, late)
        new_master, new_momentum, written, token = pl.pallas_call(
            functools.partial(write_early, plan),
            out_shape=(
                jax.ShapeDtypeStruct(state, jnp.float32),
                jax.ShapeDtypeStruct(state, jnp.float32),
                jax.ShapeDtypeStruct(layout, bf16),
                jax.ShapeDtypeStruct((8, 128), jnp.float32),
            ),
            in_specs=[any_spec] * 3,
            out_specs=(hbm_spec,) * 3 + (pl.BlockSpec(memory_space=pltpu.VMEM),),
            scratch_shapes=[
                pltpu.SemaphoreType.DMA((2,)), pltpu.SemaphoreType.DMA((K,)), pltpu.SemaphoreType.DMA((K, A)),
            ],
            compiler_params=pltpu.CompilerParams(**small),
        )(new_master, new_momentum, gathered_early)
        slots = max((A - 1) * B, A * (B - 1)) * F
        tail = pl.pallas_call(
            functools.partial(gather_late, plan),
            out_shape=pltpu.VMEM((K - min(late[:2]), slots, sub, width), bf16),
            in_specs=[any_spec] * 2,
            out_specs=any_spec,
            scratch_shapes=[pltpu.SemaphoreType.DMA((K,)), pltpu.SemaphoreType.DMA((K,))],
            compiler_params=pltpu.CompilerParams(collective_id=1, has_side_effects=True, **small),
        )(gathered_early, token)
        weights = pl.pallas_call(
            functools.partial(write_late, plan),
            out_shape=jax.ShapeDtypeStruct(layout, bf16),
            in_specs=[hbm_spec, any_spec],
            out_specs=hbm_spec,
            input_output_aliases={0: 0},
            scratch_shapes=[pltpu.SemaphoreType.DMA((K, max(A, A * (B - 1))))],
            compiler_params=pltpu.CompilerParams(**small),
        )(written, tail)
        return (new_master, new_momentum, weights.reshape(total_rows, width))

    return jax.shard_map(
        local,
        mesh=mesh,
        in_specs=(
            P("replica", None, "fsdp"),
            P("replica", "fsdp", None),
            P(("replica", "fsdp"), None),
            P(("replica", "fsdp"), None),
        ),
        out_specs=(P(("replica", "fsdp"), None), P(("replica", "fsdp"), None), P(None, "fsdp")),
        check_vma=False,
    )
```

```python
import functools

import jax
import jax.numpy as jnp
from jax import lax
from jax.experimental import pallas as pl
from jax.experimental.pallas import tpu as pltpu
from jax.sharding import PartitionSpec as P

MESH = pl.DeviceIdType.MESH

outer_rate = 0.7
momentum_factor = 0.9

LAGS = (0, 3, 6, 8, 10, 13, 13, 16)
EARLY = (10, 8, 16)
LONG = 0
TAIL = 11
RS1, RS2, X1, X2, AG1, AG2 = range(6)


def spread(even, A, B, F, a, b):
    if even:
        return [(pl.ds(a * B * F, B * F), i, pl.ds((A - 2 - i) * B * F, B * F)) for i in range(A - 1)]
    return [
        (pl.ds((aa * B + b) * F, F), i, pl.ds(((B - 2 - i) * A + aa) * F, F)) for i in range(B - 1) for aa in range(A)
    ]


def gathered(even, A, B, F, a, b):
    if even:
        return [(pl.ds(i * B * F, B * F), pl.ds(lax.rem(a + 1 + i, A) * B * F, B * F)) for i in range(A - 1)]
    return [
        (pl.ds((i * A + aa) * F, F), pl.ds((aa * B + lax.rem(b + 1 + i, B)) * F, F)) for i in range(B - 1) for aa in range(A)
    ]


def kernel(cfg, codes, scales, master, momentum, new_master, new_momentum, weights,
           delta, rs1e, rs1o, rs2e, rs2o, part, got, wsend, cbuf, flat, sbuf,
           send_sem, recv_sem, in_sem, scale_sem, state_sem, near_sem, far_sem):
    A, B, F, K, sub, width, blocks, late = cfg
    R, block, own = A * B, width // blocks, K * sub
    r, f = lax.axis_index("replica"), lax.axis_index("fsdp")
    a, b = r // B, lax.rem(r, B)
    odd_core = lax.rem(f, 2)
    held = jnp.where(odd_core == LONG, late[1], late[0])
    spread_out = jnp.where(odd_core == LONG, late[2], late[0])
    partner = (r, f + 1 - 2 * odd_core)

    def a_peer(i):
        return lax.rem(a + 1 + i, A)

    def b_peer(i):
        return lax.rem(b + 1 + i, B)

    def f_peer(i):
        return lax.rem(f + 1 + i, F)

    barrier = pltpu.get_barrier_semaphore()
    corner = R - 1
    is_corner = r == corner
    even_f = f - odd_core
    near = [(a_peer(i) * B + b) for i in range(A - 1)] + [(a * B + b_peer(i)) for i in range(B - 1)]
    for peer in near:
        device = (peer, jnp.where(peer == corner, even_f + 1, f))
        pl.semaphore_signal(barrier, inc=1, device_id=device, device_id_type=MESH)

    @pl.when(is_corner & (odd_core == 0))
    def _():
        pl.semaphore_signal(barrier, inc=1, device_id=partner, device_id_type=MESH)

    def offsets(even, p):
        if even:
            return lax.rem(1 + lax.rem(p, A), A), lax.rem(1 + p // A, B)
        return lax.rem(1 + p // B, A), lax.rem(1 + lax.rem(p, B), B)

    def at(da, db):
        return lax.rem(a + da, A) * B + lax.rem(b + db, B)

    def load(k, q):
        slot, group = lax.rem(k, 2), pl.ds(q * F, F)
        return pltpu.make_async_copy(codes.at[group, k], cbuf.at[slot, group], in_sem.at[slot, q])

    def scales_in(q):
        group = pl.ds(q * F * own, F * own)
        return pltpu.make_async_copy(scales.at[0, :, group], flat.at[pl.ds(0, blocks), group], scale_sem.at[q])

    first = tuple(
        (k, p, ((1 + p % A) % A, (1 + p // A) % B) if k == 0 else ((1 + p // B) % A, (1 + p % B) % B))
        for p in range(R) for k in range(min(2, K))
    )
    seen = set()
    for k, p, spot in first:
        if spot not in seen:
            seen.add(spot)
            scales_in(at(*spot)).start()
        load(k, at(*spot)).start()

    for i in range(F // 2 - 1):
        pair = lax.rem(f // 2 + 1 + i, F // 2)
        pl.semaphore_signal(barrier, inc=1, device_id=(corner, 2 * pair), device_id_type=MESH)

    @pl.when(jnp.logical_not(is_corner) | (odd_core == 1))
    def _():
        pl.semaphore_signal(barrier, inc=1, device_id=(corner, even_f), device_id_type=MESH)

    state_in = (
        pltpu.make_async_copy(master, new_master, state_sem.at[0]),
        pltpu.make_async_copy(momentum, new_momentum, state_sem.at[1]),
    )

    def turn(i):
        span = pl.ds(pl.multiple_of(i * 128, 128), 128)
        sbuf[span, :] = jnp.transpose(flat[:, span])

    def send(stage, k, src, dst, device):
        pltpu.make_async_remote_copy(
            src_ref=src, dst_ref=dst, send_sem=send_sem.at[stage, k], recv_sem=recv_sem.at[stage, k],
            device_id=device, device_id_type=MESH,
        ).start()

    def wait_bytes(sem, stage, k, ref):
        pltpu.make_async_copy(ref, ref, sem.at[stage, k]).wait()

    def rows(j):
        return pl.ds(pl.multiple_of(j * sub, sub), sub)

    def f32(x):
        return x.astype(jnp.float32)

    def amount(stage, k, even):
        if stage == RS1:
            return rs1e.at[k // 2] if even else rs1o.at[k // 2]
        if stage == RS2:
            return rs2e.at[k // 2] if even else rs2o.at[k // 2]
        if stage in (X1, X2):
            return part.at[k, pl.ds(0, (F - 1) * sub)]
        first, second = (B - 1, B * (A - 1)) if even else (A - 1, A * (B - 1))
        count = first if stage == AG1 else second
        return delta.at[k, pl.ds(0, count)]

    def by_parity(k, fn):
        @pl.when(lax.rem(k, 2) == 0)
        def _():
            fn(True)

        if K > 1:
            @pl.when(lax.rem(k, 2) == 1)
            def _():
                fn(False)

    def turn_scales(k, q):
        each, tiles = (F, own // 128) if own % 128 == 0 else (F * own // 128, 1)
        part = k * sub // 128 if own % 128 == 0 else 0

        def some(j, carry):
            turn((q * each + j) * tiles + part)
            return carry

        lax.fori_loop(0, each, some, 0, unroll=8)

    def scale_piece(k, q):
        slot = lax.rem(k, 2)
        load(k, q).wait()

        def one(j, carry):
            g = q * F + j
            for n in range(blocks):
                cols = pl.ds(n * block, block)
                value = f32(cbuf[slot, g, :, cols]) * sbuf[rows(g * K + k), pl.ds(n, 1)]
                delta[k, q, rows(j), cols] = value.astype(jnp.bfloat16)
            return carry

        lax.fori_loop(0, F, one, 0, unroll=4)

    def send_even(k, p, q):
        i, aa = p // A, q // B
        send(RS1, k, delta.at[k, q], rs1e.at[k // 2, B - 2 - i, aa], (a * B + lax.rem(q, B), f))

    def send_odd(k, p, q):
        i, bb = p // B, lax.rem(q, B)
        send(RS1, k, delta.at[k, q], rs1o.at[k // 2, A - 2 - i, bb], ((q // B) * B + b, f))

    def refill(k):
        @pl.when(k + 2 < K)
        def _():
            for q in range(R):
                load(k + 2, q).start()

    def begin():
        seen = set()
        for n, (k, p, spot) in enumerate(first):
            q = at(*spot)
            if spot not in seen:
                seen.add(spot)
                scales_in(q).wait()
                turn_scales(0, q)
            scale_piece(k, q)
            if n == 0:
                @pl.when(jnp.logical_not(is_corner))
                def _():
                    pl.semaphore_wait(barrier, A + B - 2)

                @pl.when(is_corner & (odd_core == 1))
                def _():
                    pl.semaphore_wait(barrier, 2 * (A + B - 2) + 1)
                    pl.semaphore_signal(near_sem, inc=1, device_id=partner, device_id_type=MESH)

                @pl.when(is_corner & (odd_core == 0))
                def _():
                    pl.semaphore_wait(near_sem, 1)

            if k == 0 and p < A * (B - 1):
                send_even(k, p, q)
            if k == 1 and p < B * (A - 1):
                send_odd(k, p, q)
        for k in range(min(2, K)):
            refill(k)
        for copy in state_in:
            copy.start()

    def stage0(k):
        def piece(even, p, carry):
            q = at(*offsets(even, p))
            if own % 128 == 0:
                @pl.when(lax.rem(k, 128 // sub) == 0)
                def _():
                    turn_scales(k, q)

            scale_piece(k, q)

            @pl.when(p < (A * (B - 1) if even else B * (A - 1)))
            def _():
                (send_even if even else send_odd)(k, p, q)

            return carry

        by_parity(k, lambda even: lax.fori_loop(0, R, functools.partial(piece, even), 0))
        refill(k)

    def stage1(k):
        def go(even):
            wait_bytes(recv_sem, RS1, k, amount(RS1, k, even))
            buf, count, peers = (rs1e, B - 1, A - 1) if even else (rs1o, A - 1, B - 1)
            for i in range(peers):
                q = a_peer(i) if even else b_peer(i)
                target = q * B + b if even else a * B + q

                def add(j, carry):
                    total = f32(delta[k, target, rows(j), :])
                    for s in range(count):
                        total = total + f32(buf[k // 2, s, q, rows(j), :])
                    buf[k // 2, 0, q, rows(j), :] = total.astype(jnp.bfloat16)
                    return carry

                lax.fori_loop(0, F, add, 0, unroll=4)
                dst = rs2e if even else rs2o
                send(RS2, k, buf.at[k // 2, 0, q], dst.at[k // 2, peers - 1 - i], (target, f))

        by_parity(k, go)

    def stage2(k):
        def go(even):
            wait_bytes(recv_sem, RS2, k, amount(RS2, k, even))
            one, two = (rs1e, rs2e) if even else (rs1o, rs2o)
            ones, twos = (B - 1, A - 1) if even else (A - 1, B - 1)
            q = a if even else b

            def add(j, carry):
                total = f32(delta[k, r, rows(j), :])
                for s in range(ones):
                    total = total + f32(one[k // 2, s, q, rows(j), :])
                for s in range(twos):
                    total = total + f32(two[k // 2, s, rows(j), :])
                part[k, rows(j), :] = total.astype(jnp.bfloat16)
                return carry

            lax.fori_loop(0, F, add, 0, unroll=4)

        by_parity(k, go)

        @pl.when((k == 0) & is_corner & (odd_core == 0))
        def _():
            pl.semaphore_wait(barrier, R * F - 1)
            for q in range(R - 1):
                for c in range(2):
                    pl.semaphore_signal(far_sem, inc=1, device_id=(q, f + c), device_id_type=MESH)
            pl.semaphore_signal(far_sem, inc=1, device_id=partner, device_id_type=MESH)

        @pl.when((k == 0) & (jnp.logical_not(is_corner) | (odd_core == 1)))
        def _():
            pl.semaphore_wait(far_sem, 1)

        def out(i, carry):
            j = f_peer(i)
            send(X1, k, part.at[k, rows(j)], got.at[k, rows(f)], (r, j))
            return carry

        lax.fori_loop(0, F - 1, out, 0)
        got[k, rows(f), :] = part[k, rows(f), :]

    def stage3(k):
        @pl.when(k == 0)
        def _():
            for copy in state_in:
                copy.wait()

        wait_bytes(recv_sem, X1, k, amount(X1, k, True))
        span = pl.ds(pl.multiple_of(k * sub, sub), sub)

        def update(j, carry):
            cols = pl.ds(pl.multiple_of(j * width, width), width)
            mean = f32(got[k, rows(j), :]) * (1.0 / R)
            m = momentum_factor * new_momentum[span, cols] + mean
            p = new_master[span, cols] - outer_rate * (mean + momentum_factor * m)
            new_momentum[span, cols] = m
            new_master[span, cols] = p
            wsend[k, rows(j), :] = p.astype(jnp.bfloat16)
            return carry

        lax.fori_loop(0, F, update, 0, unroll=4)

        def out(i, carry):
            j = f_peer(i)
            send(X2, k, wsend.at[k, rows(j)], weights.at[r * F + f, k], (r, j))
            return carry

        lax.fori_loop(0, F - 1, out, 0)
        weights[r * F + f, k, :, :] = wsend[k, rows(f), :]

    def stage4(k):
        wait_bytes(recv_sem, X2, k, amount(X2, k, True))

        def go(even):
            here = weights.at[pl.ds(r * F, F), k]
            for i in range(B - 1 if even else A - 1):
                target = a * B + b_peer(i) if even else a_peer(i) * B + b
                send(AG1, k, here, here, (target, f))

        by_parity(k, go)

    def stage5(k):
        by_parity(k, lambda even: wait_bytes(recv_sem, AG1, k, amount(AG1, k, even)))

    def gather_on(k):
        def go(even):
            for source, i, spot in spread(even, A, B, F, a, b):
                here = weights.at[source, k]
                send(AG2, k, here, here, ((a_peer(i) * B + b, f) if even else (a * B + b_peer(i), f)))

        by_parity(k, go)

    def gather_end(k):
        def go(even):
            wait_bytes(recv_sem, AG2, k, amount(AG2, k, even))
            wait_bytes(send_sem, AG2, k, amount(AG2, k, even))

        by_parity(k, go)

    def stage6(k):
        pl.when((k < spread_out) | ((k > K - 1 + TAIL - LAGS[6]) & (k < held)))(lambda: gather_on(k))

    def stage7(k):
        def go(even):
            for stage in range(5):
                wait_bytes(send_sem, stage, k, amount(stage, k, even))

        by_parity(k, go)
        pl.when(k < spread_out)(lambda: gather_end(k))

    stages = (stage0, stage1, stage2, stage3, stage4, stage5, stage6, stage7)

    def loop(fn, end):
        def one(k, carry):
            fn(k)
            return carry

        lax.fori_loop(spread_out, end, one, 0)

    def step(t, carry):
        for lag, stage in zip(LAGS, stages):
            k = t - lag

            @pl.when((k >= (min(2, K) if stage is stage0 else 0)) & (k < K))
            def _():
                stage(k)

        @pl.when(t == K - 1 + TAIL)
        def _():
            loop(gather_on, jnp.minimum(held, max(0, K + TAIL - LAGS[6])))

        return carry

    begin()
    lax.fori_loop(0, K + LAGS[-1], step, 0)
    loop(gather_end, held)


def position(cfg):
    A, B, F, K, late = cfg
    r, f = lax.axis_index("replica"), lax.axis_index("fsdp")
    return r // B, lax.rem(r, B), f, jnp.where(lax.rem(f, 2) == LONG, late[1], late[0])


def gather_late(cfg, weights, token, tail, send_sem, recv_sem):
    A, B, F, K, late = cfg
    a, b, f, held = position(cfg)
    barrier = pltpu.get_barrier_semaphore()
    peers = [(lax.rem(a + 1 + i, A) * B + b, f) for i in range(A - 1)]
    peers += [(a * B + lax.rem(b + 1 + i, B), f) for i in range(B - 1)]
    for peer in peers:
        pl.semaphore_signal(barrier, inc=1, device_id=peer, device_id_type=MESH)
    pl.semaphore_wait(barrier, A + B - 2)

    def each(fn):
        def one(k, carry):
            for even in (True, False):
                @pl.when(lax.rem(k, 2) == (0 if even else 1))
                def _():
                    fn(k, even)

            return carry

        lax.fori_loop(held, K, one, 0)

    def start(k, even):
        for source, i, slot in spread(even, A, B, F, a, b):
            pltpu.make_async_remote_copy(
                src_ref=weights.at[source, k], dst_ref=tail.at[k - min(late[:2]), slot],
                send_sem=send_sem.at[k], recv_sem=recv_sem.at[k],
                device_id=peers[i] if even else peers[A - 1 + i], device_id_type=MESH,
            ).start()

    def finish(k, even):
        moved = tail.at[k - min(late[:2]), pl.ds(0, ((A - 1) * B if even else A * (B - 1)) * F)]
        pltpu.make_async_copy(moved, moved, recv_sem.at[k]).wait()
        pltpu.make_async_copy(moved, moved, send_sem.at[k]).wait()

    each(start)
    each(finish)


def write_early(cfg, master, momentum, weights, new_master, new_momentum, written, token, state_sem, sem, late_sem):
    A, B, F, K, late = cfg
    a, b, f, held = position(cfg)
    copies = [
        pltpu.make_async_copy(master, new_master, state_sem.at[0]),
        pltpu.make_async_copy(momentum, new_momentum, state_sem.at[1]),
    ]
    for copy in copies:
        copy.start()

    def each(act):
        for k in range(K):
            if k < max(late[:2]):
                def whole(k=k):
                    act(pltpu.make_async_copy(weights.at[:, k], written.at[:, k], sem.at[k]))

                pl.when(k < held)(whole)
            if k >= min(late[:2]):
                def mine(k=k):
                    group = [pl.ds(a * B * F, B * F)] if k % 2 == 0 else [pl.ds((aa * B + b) * F, F) for aa in range(A)]
                    for n, blocks in enumerate(group):
                        act(pltpu.make_async_copy(weights.at[blocks, k], written.at[blocks, k], late_sem.at[k, n]))

                pl.when(k >= held)(mine)

    each(lambda copy: copy.start())
    token[...] = jnp.zeros_like(token)
    each(lambda copy: copy.wait())
    for copy in copies:
        copy.wait()


def write_late(cfg, written, tail, weights, sem):
    A, B, F, K, late = cfg
    a, b, f, held = position(cfg)

    def each(act):
        for k in range(min(late[:2]), K):
            def piece(k=k):
                for n, (slot, blocks) in enumerate(gathered(k % 2 == 0, A, B, F, a, b)):
                    act(pltpu.make_async_copy(tail.at[k - min(late[:2]), slot], weights.at[blocks, k], sem.at[k, n]))

            pl.when(k >= held)(piece)

    each(lambda copy: copy.start())
    each(lambda copy: copy.wait())


def solution(mesh):
    R, F = mesh.shape["replica"], mesh.shape["fsdp"]
    B = 2
    A = R // B

    def local(codes, scales, master, momentum):
        total_rows, width = codes.shape[1:]
        blocks = scales.shape[1]
        own = total_rows // (R * F)
        sub = 16 if own % 16 == 0 else own
        K = own // sub
        FS = F * sub
        even, odd = (K + 1) // 2, max(1, K // 2)
        codes = codes.reshape(R * F, K, sub, width)
        lines = max(8, blocks)
        any_spec = pl.BlockSpec(memory_space=pl.ANY)
        hbm_spec = pl.BlockSpec(memory_space=pltpu.HBM)
        bf16 = jnp.bfloat16
        late = (K * EARLY[0] // 16, K * EARLY[2] // 16, K * EARLY[1] // 16)
        state, layout = master.shape, (R * F, K, sub, width)
        new_master, new_momentum, gathered_early = pl.pallas_call(
            functools.partial(kernel, (A, B, F, K, sub, width, blocks, late)),
            out_shape=(
                pltpu.VMEM(state, jnp.float32),
                pltpu.VMEM(state, jnp.float32),
                pltpu.VMEM(layout, bf16),
            ),
            in_specs=[hbm_spec] * 4,
            out_specs=(pl.BlockSpec(memory_space=pltpu.VMEM),) * 3,
            scratch_shapes=[
                pltpu.VMEM((K, R, FS, width), bf16),
                pltpu.VMEM((even, B - 1, A, FS, width), bf16),
                pltpu.VMEM((odd, A - 1, B, FS, width), bf16),
                pltpu.VMEM((even, A - 1, FS, width), bf16),
                pltpu.VMEM((odd, B - 1, FS, width), bf16),
                pltpu.VMEM((K, FS, width), bf16),
                pltpu.VMEM((K, FS, width), bf16),
                pltpu.VMEM((K, FS, width), bf16),
                pltpu.VMEM((2, R * F, sub, width), jnp.int32),
                pltpu.VMEM((lines, total_rows), jnp.float32),
                pltpu.VMEM((total_rows, lines), jnp.float32),
                pltpu.SemaphoreType.DMA((6, K)),
                pltpu.SemaphoreType.DMA((6, K)),
                pltpu.SemaphoreType.DMA((2, R)),
                pltpu.SemaphoreType.DMA((R,)),
                pltpu.SemaphoreType.DMA((2,)),
                pltpu.SemaphoreType.REGULAR,
                pltpu.SemaphoreType.REGULAR,
            ],
            compiler_params=pltpu.CompilerParams(
                collective_id=0, has_side_effects=True, vmem_limit_bytes=46 * 1024 * 1024
            ),
        )(codes, scales, master, momentum)
        small = dict(vmem_limit_bytes=1024 * 1024)
        plan = (A, B, F, K, late)
        new_master, new_momentum, written, token = pl.pallas_call(
            functools.partial(write_early, plan),
            out_shape=(
                jax.ShapeDtypeStruct(state, jnp.float32),
                jax.ShapeDtypeStruct(state, jnp.float32),
                jax.ShapeDtypeStruct(layout, bf16),
                jax.ShapeDtypeStruct((8, 128), jnp.float32),
            ),
            in_specs=[any_spec] * 3,
            out_specs=(hbm_spec,) * 3 + (pl.BlockSpec(memory_space=pltpu.VMEM),),
            scratch_shapes=[
                pltpu.SemaphoreType.DMA((2,)), pltpu.SemaphoreType.DMA((K,)), pltpu.SemaphoreType.DMA((K, A)),
            ],
            compiler_params=pltpu.CompilerParams(**small),
        )(new_master, new_momentum, gathered_early)
        slots = max((A - 1) * B, A * (B - 1)) * F
        tail = pl.pallas_call(
            functools.partial(gather_late, plan),
            out_shape=pltpu.VMEM((K - min(late[:2]), slots, sub, width), bf16),
            in_specs=[any_spec] * 2,
            out_specs=any_spec,
            scratch_shapes=[pltpu.SemaphoreType.DMA((K,)), pltpu.SemaphoreType.DMA((K,))],
            compiler_params=pltpu.CompilerParams(collective_id=1, has_side_effects=True, **small),
        )(gathered_early, token)
        weights = pl.pallas_call(
            functools.partial(write_late, plan),
            out_shape=jax.ShapeDtypeStruct(layout, bf16),
            in_specs=[hbm_spec, any_spec],
            out_specs=hbm_spec,
            input_output_aliases={0: 0},
            scratch_shapes=[pltpu.SemaphoreType.DMA((K, max(A, A * (B - 1))))],
            compiler_params=pltpu.CompilerParams(**small),
        )(written, tail)
        return (new_master, new_momentum, weights.reshape(total_rows, width))

    return jax.shard_map(
        local,
        mesh=mesh,
        in_specs=(
            P("replica", None, "fsdp"),
            P("replica", "fsdp", None),
            P(("replica", "fsdp"), None),
            P(("replica", "fsdp"), None),
        ),
        out_specs=(P(("replica", "fsdp"), None), P(("replica", "fsdp"), None), P(None, "fsdp")),
        check_vma=False,
    )
```

```python
import functools

import jax
import jax.numpy as jnp
from jax import lax
from jax.experimental import pallas as pl
from jax.experimental.pallas import tpu as pltpu
from jax.sharding import PartitionSpec as P

MESH = pl.DeviceIdType.MESH

outer_rate = 0.7
momentum_factor = 0.9

LAGS = (0, 3, 6, 8, 10, 13, 13, 16)
EARLY = (10, 8, 16)
LONG = 0
TAIL = 11
RS1, RS2, X1, X2, AG1, AG2 = range(6)


def spread(even, A, B, F, a, b):
    if even:
        return [(pl.ds(a * B * F, B * F), i, pl.ds((A - 2 - i) * B * F, B * F)) for i in range(A - 1)]
    return [
        (pl.ds((aa * B + b) * F, F), i, pl.ds(((B - 2 - i) * A + aa) * F, F)) for i in range(B - 1) for aa in range(A)
    ]


def gathered(even, A, B, F, a, b):
    if even:
        return [(pl.ds(i * B * F, B * F), pl.ds(lax.rem(a + 1 + i, A) * B * F, B * F)) for i in range(A - 1)]
    return [
        (pl.ds((i * A + aa) * F, F), pl.ds((aa * B + lax.rem(b + 1 + i, B)) * F, F)) for i in range(B - 1) for aa in range(A)
    ]


def kernel(cfg, codes, scales, master, momentum, new_master, new_momentum, weights,
           delta, rs1e, rs1o, rs2e, rs2o, part, got, wsend, cbuf, flat, sbuf,
           send_sem, recv_sem, in_sem, scale_sem, state_sem, near_sem, far_sem):
    A, B, F, K, sub, width, blocks, late = cfg
    R, block, own = A * B, width // blocks, K * sub
    r, f = lax.axis_index("replica"), lax.axis_index("fsdp")
    a, b = r // B, lax.rem(r, B)
    odd_core = lax.rem(f, 2)
    held = jnp.where(odd_core == LONG, late[1], late[0])
    spread_out = jnp.where(odd_core == LONG, late[2], late[0])
    partner = (r, f + 1 - 2 * odd_core)

    def a_peer(i):
        return lax.rem(a + 1 + i, A)

    def b_peer(i):
        return lax.rem(b + 1 + i, B)

    def f_peer(i):
        return lax.rem(f + 1 + i, F)

    barrier = pltpu.get_barrier_semaphore()
    corner = R - 1
    is_corner = r == corner
    even_f = f - odd_core
    near = [(a_peer(i) * B + b) for i in range(A - 1)] + [(a * B + b_peer(i)) for i in range(B - 1)]
    for peer in near:
        device = (peer, jnp.where(peer == corner, even_f + 1, f))
        pl.semaphore_signal(barrier, inc=1, device_id=device, device_id_type=MESH)

    @pl.when(is_corner & (odd_core == 0))
    def _():
        pl.semaphore_signal(barrier, inc=1, device_id=partner, device_id_type=MESH)

    def offsets(even, p):
        if even:
            return lax.rem(1 + lax.rem(p, A), A), lax.rem(1 + p // A, B)
        return lax.rem(1 + p // B, A), lax.rem(1 + lax.rem(p, B), B)

    def at(da, db):
        return lax.rem(a + da, A) * B + lax.rem(b + db, B)

    def load(k, q):
        slot, group = lax.rem(k, 2), pl.ds(q * F, F)
        return pltpu.make_async_copy(codes.at[group, k], cbuf.at[slot, group], in_sem.at[slot, q])

    def scales_in(q):
        group = pl.ds(q * F * own, F * own)
        return pltpu.make_async_copy(scales.at[0, :, group], flat.at[pl.ds(0, blocks), group], scale_sem.at[q])

    first = tuple(
        (k, p, ((1 + p % A) % A, (1 + p // A) % B) if k == 0 else ((1 + p // B) % A, (1 + p % B) % B))
        for p in range(R) for k in range(min(2, K))
    )
    opening = min(2, K)

    def fetch(pieces, seen):
        for k, p, spot in pieces:
            if spot not in seen:
                seen.add(spot)
                scales_in(at(*spot)).start()
            load(k, at(*spot)).start()

    fetch(first[:opening], set())

    for i in range(F // 2 - 1):
        pair = lax.rem(f // 2 + 1 + i, F // 2)
        pl.semaphore_signal(barrier, inc=1, device_id=(corner, 2 * pair), device_id_type=MESH)

    @pl.when(jnp.logical_not(is_corner) | (odd_core == 1))
    def _():
        pl.semaphore_signal(barrier, inc=1, device_id=(corner, even_f), device_id_type=MESH)

    state_in = (
        pltpu.make_async_copy(master, new_master, state_sem.at[0]),
        pltpu.make_async_copy(momentum, new_momentum, state_sem.at[1]),
    )

    def turn(i):
        span = pl.ds(pl.multiple_of(i * 128, 128), 128)
        sbuf[span, :] = jnp.transpose(flat[:, span])

    def send(stage, k, src, dst, device):
        pltpu.make_async_remote_copy(
            src_ref=src, dst_ref=dst, send_sem=send_sem.at[stage, k], recv_sem=recv_sem.at[stage, k],
            device_id=device, device_id_type=MESH,
        ).start()

    def wait_bytes(sem, stage, k, ref):
        pltpu.make_async_copy(ref, ref, sem.at[stage, k]).wait()

    def rows(j):
        return pl.ds(pl.multiple_of(j * sub, sub), sub)

    def f32(x):
        return x.astype(jnp.float32)

    def amount(stage, k, even):
        if stage == RS1:
            return rs1e.at[k // 2] if even else rs1o.at[k // 2]
        if stage == RS2:
            return rs2e.at[k // 2] if even else rs2o.at[k // 2]
        if stage in (X1, X2):
            return part.at[k, pl.ds(0, (F - 1) * sub)]
        first, second = (B - 1, B * (A - 1)) if even else (A - 1, A * (B - 1))
        count = first if stage == AG1 else second
        return delta.at[k, pl.ds(0, count)]

    def by_parity(k, fn):
        @pl.when(lax.rem(k, 2) == 0)
        def _():
            fn(True)

        if K > 1:
            @pl.when(lax.rem(k, 2) == 1)
            def _():
                fn(False)

    def turn_scales(k, q):
        each, tiles = (F, own // 128) if own % 128 == 0 else (F * own // 128, 1)
        part = k * sub // 128 if own % 128 == 0 else 0

        def some(j, carry):
            turn((q * each + j) * tiles + part)
            return carry

        lax.fori_loop(0, each, some, 0, unroll=8)

    def scale_piece(k, q):
        slot = lax.rem(k, 2)
        load(k, q).wait()

        def one(j, carry):
            g = q * F + j
            for n in range(blocks):
                cols = pl.ds(n * block, block)
                value = f32(cbuf[slot, g, :, cols]) * sbuf[rows(g * K + k), pl.ds(n, 1)]
                delta[k, q, rows(j), cols] = value.astype(jnp.bfloat16)
            return carry

        lax.fori_loop(0, F, one, 0, unroll=4)

    def send_even(k, p, q):
        i, aa = p // A, q // B
        send(RS1, k, delta.at[k, q], rs1e.at[k // 2, B - 2 - i, aa], (a * B + lax.rem(q, B), f))

    def send_odd(k, p, q):
        i, bb = p // B, lax.rem(q, B)
        send(RS1, k, delta.at[k, q], rs1o.at[k // 2, A - 2 - i, bb], ((q // B) * B + b, f))

    def refill(k):
        @pl.when(k + 2 < K)
        def _():
            for q in range(R):
                load(k + 2, q).start()

    def begin():
        seen = set()
        for n, (k, p, spot) in enumerate(first):
            q = at(*spot)
            if spot not in seen:
                seen.add(spot)
                scales_in(q).wait()
                turn_scales(0, q)
            scale_piece(k, q)
            if n == 0:
                fetch(first[opening:], {spot for _, _, spot in first[:opening]})

                @pl.when(jnp.logical_not(is_corner))
                def _():
                    pl.semaphore_wait(barrier, A + B - 2)

                @pl.when(is_corner & (odd_core == 1))
                def _():
                    pl.semaphore_wait(barrier, 2 * (A + B - 2) + 1)
                    pl.semaphore_signal(near_sem, inc=1, device_id=partner, device_id_type=MESH)

                @pl.when(is_corner & (odd_core == 0))
                def _():
                    pl.semaphore_wait(near_sem, 1)

            if k == 0 and p < A * (B - 1):
                send_even(k, p, q)
            if k == 1 and p < B * (A - 1):
                send_odd(k, p, q)
        for k in range(min(2, K)):
            refill(k)
        for copy in state_in:
            copy.start()

    def stage0(k):
        def piece(even, p, carry):
            q = at(*offsets(even, p))
            if own % 128 == 0:
                @pl.when(lax.rem(k, 128 // sub) == 0)
                def _():
                    turn_scales(k, q)

            scale_piece(k, q)

            @pl.when(p < (A * (B - 1) if even else B * (A - 1)))
            def _():
                (send_even if even else send_odd)(k, p, q)

            return carry

        by_parity(k, lambda even: lax.fori_loop(0, R, functools.partial(piece, even), 0))
        refill(k)

    def stage1(k):
        def go(even):
            wait_bytes(recv_sem, RS1, k, amount(RS1, k, even))
            buf, count, peers = (rs1e, B - 1, A - 1) if even else (rs1o, A - 1, B - 1)
            for i in range(peers):
                q = a_peer(i) if even else b_peer(i)
                target = q * B + b if even else a * B + q

                def add(j, carry):
                    total = f32(delta[k, target, rows(j), :])
                    for s in range(count):
                        total = total + f32(buf[k // 2, s, q, rows(j), :])
                    buf[k // 2, 0, q, rows(j), :] = total.astype(jnp.bfloat16)
                    return carry

                lax.fori_loop(0, F, add, 0, unroll=4)
                dst = rs2e if even else rs2o
                send(RS2, k, buf.at[k // 2, 0, q], dst.at[k // 2, peers - 1 - i], (target, f))

        by_parity(k, go)

    def stage2(k):
        def go(even):
            wait_bytes(recv_sem, RS2, k, amount(RS2, k, even))
            one, two = (rs1e, rs2e) if even else (rs1o, rs2o)
            ones, twos = (B - 1, A - 1) if even else (A - 1, B - 1)
            q = a if even else b

            def add(j, carry):
                total = f32(delta[k, r, rows(j), :])
                for s in range(ones):
                    total = total + f32(one[k // 2, s, q, rows(j), :])
                for s in range(twos):
                    total = total + f32(two[k // 2, s, rows(j), :])
                part[k, rows(j), :] = total.astype(jnp.bfloat16)
                return carry

            lax.fori_loop(0, F, add, 0, unroll=4)

        by_parity(k, go)

        @pl.when((k == 0) & is_corner & (odd_core == 0))
        def _():
            pl.semaphore_wait(barrier, R * F - 1)
            for q in range(R - 1):
                for c in range(2):
                    pl.semaphore_signal(far_sem, inc=1, device_id=(q, f + c), device_id_type=MESH)
            pl.semaphore_signal(far_sem, inc=1, device_id=partner, device_id_type=MESH)

        @pl.when((k == 0) & (jnp.logical_not(is_corner) | (odd_core == 1)))
        def _():
            pl.semaphore_wait(far_sem, 1)

        def out(i, carry):
            j = f_peer(i)
            send(X1, k, part.at[k, rows(j)], got.at[k, rows(f)], (r, j))
            return carry

        lax.fori_loop(0, F - 1, out, 0)
        got[k, rows(f), :] = part[k, rows(f), :]

    def stage3(k):
        @pl.when(k == 0)
        def _():
            for copy in state_in:
                copy.wait()

        wait_bytes(recv_sem, X1, k, amount(X1, k, True))
        span = pl.ds(pl.multiple_of(k * sub, sub), sub)

        def update(j, carry):
            cols = pl.ds(pl.multiple_of(j * width, width), width)
            mean = f32(got[k, rows(j), :]) * (1.0 / R)
            m = momentum_factor * new_momentum[span, cols] + mean
            p = new_master[span, cols] - outer_rate * (mean + momentum_factor * m)
            new_momentum[span, cols] = m
            new_master[span, cols] = p
            wsend[k, rows(j), :] = p.astype(jnp.bfloat16)
            return carry

        lax.fori_loop(0, F, update, 0, unroll=4)

        def out(i, carry):
            j = f_peer(i)
            send(X2, k, wsend.at[k, rows(j)], weights.at[r * F + f, k], (r, j))
            return carry

        lax.fori_loop(0, F - 1, out, 0)
        weights[r * F + f, k, :, :] = wsend[k, rows(f), :]

    def stage4(k):
        wait_bytes(recv_sem, X2, k, amount(X2, k, True))

        def go(even):
            here = weights.at[pl.ds(r * F, F), k]
            for i in range(B - 1 if even else A - 1):
                target = a * B + b_peer(i) if even else a_peer(i) * B + b
                send(AG1, k, here, here, (target, f))

        by_parity(k, go)

    def stage5(k):
        by_parity(k, lambda even: wait_bytes(recv_sem, AG1, k, amount(AG1, k, even)))

    def gather_on(k):
        def go(even):
            for source, i, spot in spread(even, A, B, F, a, b):
                here = weights.at[source, k]
                send(AG2, k, here, here, ((a_peer(i) * B + b, f) if even else (a * B + b_peer(i), f)))

        by_parity(k, go)

    def gather_end(k):
        def go(even):
            wait_bytes(recv_sem, AG2, k, amount(AG2, k, even))
            wait_bytes(send_sem, AG2, k, amount(AG2, k, even))

        by_parity(k, go)

    def stage6(k):
        pl.when((k < spread_out) | ((k > K - 1 + TAIL - LAGS[6]) & (k < held)))(lambda: gather_on(k))

    def stage7(k):
        def go(even):
            for stage in range(5):
                wait_bytes(send_sem, stage, k, amount(stage, k, even))

        by_parity(k, go)
        pl.when(k < spread_out)(lambda: gather_end(k))

    stages = (stage0, stage1, stage2, stage3, stage4, stage5, stage6, stage7)

    def loop(fn, end):
        def one(k, carry):
            fn(k)
            return carry

        lax.fori_loop(spread_out, end, one, 0)

    def step(t, carry):
        for lag, stage in zip(LAGS, stages):
            k = t - lag

            @pl.when((k >= (min(2, K) if stage is stage0 else 0)) & (k < K))
            def _():
                stage(k)

        @pl.when(t == K - 1 + TAIL)
        def _():
            loop(gather_on, jnp.minimum(held, max(0, K + TAIL - LAGS[6])))

        return carry

    begin()
    lax.fori_loop(0, K + LAGS[-1], step, 0)
    loop(gather_end, held)


def position(cfg):
    A, B, F, K, late = cfg
    r, f = lax.axis_index("replica"), lax.axis_index("fsdp")
    return r // B, lax.rem(r, B), f, jnp.where(lax.rem(f, 2) == LONG, late[1], late[0])


def gather_late(cfg, weights, token, tail, send_sem, recv_sem):
    A, B, F, K, late = cfg
    a, b, f, held = position(cfg)
    barrier = pltpu.get_barrier_semaphore()
    peers = [(lax.rem(a + 1 + i, A) * B + b, f) for i in range(A - 1)]
    peers += [(a * B + lax.rem(b + 1 + i, B), f) for i in range(B - 1)]
    for peer in peers:
        pl.semaphore_signal(barrier, inc=1, device_id=peer, device_id_type=MESH)
    pl.semaphore_wait(barrier, A + B - 2)

    def each(fn):
        def one(k, carry):
            for even in (True, False):
                @pl.when(lax.rem(k, 2) == (0 if even else 1))
                def _():
                    fn(k, even)

            return carry

        lax.fori_loop(held, K, one, 0)

    def start(k, even):
        for source, i, slot in spread(even, A, B, F, a, b):
            pltpu.make_async_remote_copy(
                src_ref=weights.at[source, k], dst_ref=tail.at[k - min(late[:2]), slot],
                send_sem=send_sem.at[k], recv_sem=recv_sem.at[k],
                device_id=peers[i] if even else peers[A - 1 + i], device_id_type=MESH,
            ).start()

    def finish(k, even):
        moved = tail.at[k - min(late[:2]), pl.ds(0, ((A - 1) * B if even else A * (B - 1)) * F)]
        pltpu.make_async_copy(moved, moved, recv_sem.at[k]).wait()
        pltpu.make_async_copy(moved, moved, send_sem.at[k]).wait()

    each(start)
    each(finish)


def write_early(cfg, master, momentum, weights, new_master, new_momentum, written, token, state_sem, sem, late_sem):
    A, B, F, K, late = cfg
    a, b, f, held = position(cfg)
    copies = [
        pltpu.make_async_copy(master, new_master, state_sem.at[0]),
        pltpu.make_async_copy(momentum, new_momentum, state_sem.at[1]),
    ]
    for copy in copies:
        copy.start()

    def each(act):
        for k in range(K):
            if k < max(late[:2]):
                def whole(k=k):
                    act(pltpu.make_async_copy(weights.at[:, k], written.at[:, k], sem.at[k]))

                pl.when(k < held)(whole)
            if k >= min(late[:2]):
                def mine(k=k):
                    group = [pl.ds(a * B * F, B * F)] if k % 2 == 0 else [pl.ds((aa * B + b) * F, F) for aa in range(A)]
                    for n, blocks in enumerate(group):
                        act(pltpu.make_async_copy(weights.at[blocks, k], written.at[blocks, k], late_sem.at[k, n]))

                pl.when(k >= held)(mine)

    each(lambda copy: copy.start())
    token[...] = jnp.zeros_like(token)
    each(lambda copy: copy.wait())
    for copy in copies:
        copy.wait()


def write_late(cfg, written, tail, weights, sem):
    A, B, F, K, late = cfg
    a, b, f, held = position(cfg)

    def each(act):
        for k in range(min(late[:2]), K):
            def piece(k=k):
                for n, (slot, blocks) in enumerate(gathered(k % 2 == 0, A, B, F, a, b)):
                    act(pltpu.make_async_copy(tail.at[k - min(late[:2]), slot], weights.at[blocks, k], sem.at[k, n]))

            pl.when(k >= held)(piece)

    each(lambda copy: copy.start())
    each(lambda copy: copy.wait())


def solution(mesh):
    R, F = mesh.shape["replica"], mesh.shape["fsdp"]
    B = 2
    A = R // B

    def local(codes, scales, master, momentum):
        total_rows, width = codes.shape[1:]
        blocks = scales.shape[1]
        own = total_rows // (R * F)
        sub = 16 if own % 16 == 0 else own
        K = own // sub
        FS = F * sub
        even, odd = (K + 1) // 2, max(1, K // 2)
        codes = codes.reshape(R * F, K, sub, width)
        lines = max(8, blocks)
        any_spec = pl.BlockSpec(memory_space=pl.ANY)
        hbm_spec = pl.BlockSpec(memory_space=pltpu.HBM)
        bf16 = jnp.bfloat16
        late = (K * EARLY[0] // 16, K * EARLY[2] // 16, K * EARLY[1] // 16)
        state, layout = master.shape, (R * F, K, sub, width)
        new_master, new_momentum, gathered_early = pl.pallas_call(
            functools.partial(kernel, (A, B, F, K, sub, width, blocks, late)),
            out_shape=(
                pltpu.VMEM(state, jnp.float32),
                pltpu.VMEM(state, jnp.float32),
                pltpu.VMEM(layout, bf16),
            ),
            in_specs=[hbm_spec] * 4,
            out_specs=(pl.BlockSpec(memory_space=pltpu.VMEM),) * 3,
            scratch_shapes=[
                pltpu.VMEM((K, R, FS, width), bf16),
                pltpu.VMEM((even, B - 1, A, FS, width), bf16),
                pltpu.VMEM((odd, A - 1, B, FS, width), bf16),
                pltpu.VMEM((even, A - 1, FS, width), bf16),
                pltpu.VMEM((odd, B - 1, FS, width), bf16),
                pltpu.VMEM((K, FS, width), bf16),
                pltpu.VMEM((K, FS, width), bf16),
                pltpu.VMEM((K, FS, width), bf16),
                pltpu.VMEM((2, R * F, sub, width), jnp.int32),
                pltpu.VMEM((lines, total_rows), jnp.float32),
                pltpu.VMEM((total_rows, lines), jnp.float32),
                pltpu.SemaphoreType.DMA((6, K)),
                pltpu.SemaphoreType.DMA((6, K)),
                pltpu.SemaphoreType.DMA((2, R)),
                pltpu.SemaphoreType.DMA((R,)),
                pltpu.SemaphoreType.DMA((2,)),
                pltpu.SemaphoreType.REGULAR,
                pltpu.SemaphoreType.REGULAR,
            ],
            compiler_params=pltpu.CompilerParams(
                collective_id=0, has_side_effects=True, vmem_limit_bytes=46 * 1024 * 1024
            ),
        )(codes, scales, master, momentum)
        small = dict(vmem_limit_bytes=1024 * 1024)
        plan = (A, B, F, K, late)
        new_master, new_momentum, written, token = pl.pallas_call(
            functools.partial(write_early, plan),
            out_shape=(
                jax.ShapeDtypeStruct(state, jnp.float32),
                jax.ShapeDtypeStruct(state, jnp.float32),
                jax.ShapeDtypeStruct(layout, bf16),
                jax.ShapeDtypeStruct((8, 128), jnp.float32),
            ),
            in_specs=[any_spec] * 3,
            out_specs=(hbm_spec,) * 3 + (pl.BlockSpec(memory_space=pltpu.VMEM),),
            scratch_shapes=[
                pltpu.SemaphoreType.DMA((2,)), pltpu.SemaphoreType.DMA((K,)), pltpu.SemaphoreType.DMA((K, A)),
            ],
            compiler_params=pltpu.CompilerParams(**small),
        )(new_master, new_momentum, gathered_early)
        slots = max((A - 1) * B, A * (B - 1)) * F
        tail = pl.pallas_call(
            functools.partial(gather_late, plan),
            out_shape=pltpu.VMEM((K - min(late[:2]), slots, sub, width), bf16),
            in_specs=[any_spec] * 2,
            out_specs=any_spec,
            scratch_shapes=[pltpu.SemaphoreType.DMA((K,)), pltpu.SemaphoreType.DMA((K,))],
            compiler_params=pltpu.CompilerParams(collective_id=1, has_side_effects=True, **small),
        )(gathered_early, token)
        weights = pl.pallas_call(
            functools.partial(write_late, plan),
            out_shape=jax.ShapeDtypeStruct(layout, bf16),
            in_specs=[hbm_spec, any_spec],
            out_specs=hbm_spec,
            input_output_aliases={0: 0},
            scratch_shapes=[pltpu.SemaphoreType.DMA((K, max(A, A * (B - 1))))],
            compiler_params=pltpu.CompilerParams(**small),
        )(written, tail)
        return (new_master, new_momentum, weights.reshape(total_rows, width))

    return jax.shard_map(
        local,
        mesh=mesh,
        in_specs=(
            P("replica", None, "fsdp"),
            P("replica", "fsdp", None),
            P(("replica", "fsdp"), None),
            P(("replica", "fsdp"), None),
        ),
        out_specs=(P(("replica", "fsdp"), None), P(("replica", "fsdp"), None), P(None, "fsdp")),
        check_vma=False,
    )
```
